32 devices in a mesh: space: 8 (over y, x, core), tm: 4 (over z).
Axes of the slice: x: 2, y: 2, z: 4, core: 2. Of those that a mesh axis runs over, the one named last changes fastest.
Arguments:
- links: float32 [4, 3, 2, 3, 3, 16, 4096], P('tm', None, None, None, None, 'space'), may hold values from -1 to 1, as said below
- propagator: float32 [2, 144, 16, 4096], P(None, 'tm', 'space'), may hold values from -6 to 6
- sink_time: int32 [1], replicated, may hold values from 0 to 16383
- src_time: int32 [1], replicated, may hold values from 0 to 16383
- src_site: int32 [1], replicated, may hold values from 0 to 65535
Outputs:
- fixed_links: float32 [4, 3, 2, 3, 3, 16, 4096], P('tm', None, None, None, None, 'space')
- wall: float32 [2, 144], replicated
The draws below stay inside these ranges and needn't reach their ends.
Inputs may be any that keep to these rules, and one draw needn't show every extreme that they name: `links`: every link is a special unitary 3 x 3 matrix up to rounding.
All inputs are finite; a program needn't handle non-finite values.
Results may differ from the reference program's by a relative error of at most 0.0001.
Values sent between devices are 32-bit elements; how exact they have to be, the bound alone decides.
A program may use at most 128 MiB of HBM per device.

```python
import math
import jax
import jax.numpy as jnp
from jax import lax

L = 64
SC = 12
ITERS = 2
NX = 16
NT = 4


def draw_product(left_matrix, right_matrix):
    pattern = 'tdikxn,tdkjxn->tdijxn'
    real_part = jnp.einsum(pattern, left_matrix[:, :, 0], right_matrix[:, :, 0]) - jnp.einsum(pattern, left_matrix[:, :, 1], right_matrix[:, :, 1])
    imag_part = jnp.einsum(pattern, left_matrix[:, :, 0], right_matrix[:, :, 1]) + jnp.einsum(pattern, left_matrix[:, :, 1], right_matrix[:, :, 0])
    return jnp.stack([real_part, imag_part], axis=2)


def draw_links(key, part):
    normal_draw = jax.random.normal(key, (NT, 3, 2, 3, 3, NX, L * L), jnp.float32)
    real_part = normal_draw[:, :, 0]
    imag_part = normal_draw[:, :, 1]
    real_anti = 0.5 * (real_part - jnp.swapaxes(real_part, 2, 3))
    imag_sym = 0.5 * (imag_part + jnp.swapaxes(imag_part, 2, 3))
    trace_third = (imag_sym[:, :, 0, 0] + imag_sym[:, :, 1, 1] + imag_sym[:, :, 2, 2]) / 3.0
    unit_matrix = jnp.eye(3, dtype=jnp.float32)[None, None, :, :, None, None]
    imag_sym = imag_sym - unit_matrix * trace_third[:, :, None, None]
    algebra = jnp.stack([real_anti, imag_sym], axis=2) / 16.0
    identity = jnp.stack([jnp.broadcast_to(unit_matrix, real_anti.shape), jnp.zeros(real_anti.shape, jnp.float32)], axis=2)
    result = identity
    for degree in range(8, 0, -1):
        result = identity + draw_product(algebra, result) / degree
    for square_index in range(4):
        result = draw_product(result, result)
    return result


def level_of(rng, extent, shards, least, largest):
    def one(axis_at, shards_of):
        heights = jax.random.uniform(jax.random.fold_in(jax.random.fold_in(rng, 6), axis_at), (shards_of,), jnp.float32, least / len(shards), largest / len(shards))
        return jnp.repeat(jnp.exp(heights), extent[axis_at] // shards_of).reshape((-1,) + (1,) * (len(extent) - axis_at - 1))

    level = one(*shards[0])
    for cut in shards[1:]:
        level = level * one(*cut)
    return level


def noise(key, shape, scale, reach, cuts=(), kind=jnp.bfloat16):
    entries = scale * jax.random.normal(key, shape, jnp.float32)
    if cuts:
        entries = entries * level_of(key, shape, cuts, -0.22, 0.18)
    return jnp.clip(entries, -reach, reach).astype(kind)


def setup_inputs(seed: int = 0) -> dict:
    arg_keys = jax.random.split(jax.random.key(seed), 6)
    links = draw_links(jax.random.fold_in(arg_keys[5], 71), 0)
    propagator = noise(arg_keys[1], (2, SC * SC, NX, L * L), 1.0, 6.0, ((1, 4), (2, 8)), jnp.float32)
    sink_time = jax.random.randint(arg_keys[2], (1,), 0, NT * 4096).astype(jnp.int32)
    src_time = jax.random.randint(arg_keys[3], (1,), 0, NT * 4096).astype(jnp.int32)
    src_site = jax.random.randint(arg_keys[4], (1,), 0, NX * L * L).astype(jnp.int32)
    return dict(links=links, propagator=propagator, sink_time=sink_time, src_time=src_time, src_site=src_site)


STEP_SIZE = 0.08
PEAK_SQUARE = 12.0
ENTRY_PAIRS = ((0, 0), (0, 1), (0, 2), (1, 1), (1, 2), (2, 2))
EXACT = lax.Precision.HIGHEST


def colour_product(left_matrix, right_matrix):
    return jnp.sum(left_matrix[:, :, None] * right_matrix[None, :, :], axis=1)


def complex_product(left_matrix, right_matrix):
    real_part = colour_product(left_matrix[0], right_matrix[0]) - colour_product(left_matrix[1], right_matrix[1])
    imag_part = colour_product(left_matrix[0], right_matrix[1]) + colour_product(left_matrix[1], right_matrix[0])
    return jnp.stack([real_part, imag_part])


def dagger(matrix):
    return jnp.stack([jnp.swapaxes(matrix[0], 0, 1), -jnp.swapaxes(matrix[1], 0, 1)])


def roll_depth(values, amount):
    old_shape = values.shape
    folded = values.reshape(old_shape[:-1] + (L, L))
    return jnp.roll(folded, amount, axis=-1).reshape(old_shape)


def project(divergence):
    real_part = 0.5 * (divergence[0] - jnp.swapaxes(divergence[0], 0, 1))
    imag_part = 0.5 * (divergence[1] + jnp.swapaxes(divergence[1], 0, 1))
    trace_third = (imag_part[0, 0] + imag_part[1, 1] + imag_part[2, 2]) / 3.0
    real_six = jnp.stack([real_part[row_index, column_index] for row_index, column_index in ENTRY_PAIRS])
    imag_six = jnp.stack([imag_part[row_index, column_index] - trace_third if row_index == column_index else imag_part[row_index, column_index] for row_index, column_index in ENTRY_PAIRS])
    return real_six, imag_six


def assemble(real_six, imag_six):
    zero_plane = jnp.zeros_like(real_six[0])
    position = {}
    for entry_index, entry_pair in enumerate(ENTRY_PAIRS):
        position[entry_pair] = entry_index
    real_rows = []
    imag_rows = []
    for row_index in range(3):
        real_line = []
        imag_line = []
        for column_index in range(3):
            if row_index == column_index:
                real_line.append(zero_plane)
                imag_line.append(imag_six[position[(row_index, row_index)]])
            elif row_index < column_index:
                slot_index = position[(row_index, column_index)]
                real_line.append(real_six[slot_index])
                imag_line.append(imag_six[slot_index])
            else:
                slot_index = position[(column_index, row_index)]
                real_line.append(-real_six[slot_index])
                imag_line.append(imag_six[slot_index])
        real_rows.append(jnp.stack(real_line))
        imag_rows.append(jnp.stack(imag_line))
    return jnp.stack([jnp.stack(real_rows), jnp.stack(imag_rows)])


def exponential(algebra):
    unit_matrix = jnp.eye(3, dtype=jnp.float32).reshape((3, 3) + (1,) * (algebra.ndim - 3))
    identity = jnp.stack([jnp.broadcast_to(unit_matrix, algebra.shape[1:]), jnp.zeros(algebra.shape[1:], jnp.float32)])
    result = identity
    for degree in range(6, 0, -1):
        result = identity + complex_product(algebra, result) / degree
    for square_index in range(3):
        result = complex_product(result, result)
    return result


def rotate(lattice, gauge_field, gauge_ahead):
    along_x = complex_product(complex_product(gauge_field, lattice[0]), dagger(gauge_ahead))
    along_y = complex_product(complex_product(gauge_field, lattice[1]), dagger(jnp.roll(gauge_field, -L, axis=4)))
    along_z = complex_product(complex_product(gauge_field, lattice[2]), dagger(roll_depth(gauge_field, -1)))
    return jnp.stack([along_x, along_y, along_z])


def sink_product(gauge_field, propagator):
    pair_count = propagator.shape[1]
    source = propagator.reshape((2, pair_count // 3, 3) + propagator.shape[2:])
    pattern = "acxn,qcxn->qa"
    real_part = jnp.einsum(pattern, gauge_field[0], source[0], precision=EXACT) - jnp.einsum(pattern, gauge_field[1], source[1], precision=EXACT)
    imag_part = jnp.einsum(pattern, gauge_field[0], source[1], precision=EXACT) + jnp.einsum(pattern, gauge_field[1], source[0], precision=EXACT)
    return jnp.stack([real_part.reshape(pair_count), imag_part.reshape(pair_count)])


def source_rotate(wall_total, anchor):
    by_spin = wall_total.reshape(2, 4, 3, SC)
    pattern = "scn,bc->sbn"
    real_part = jnp.einsum(pattern, by_spin[0], anchor[0], precision=EXACT) + jnp.einsum(pattern, by_spin[1], anchor[1], precision=EXACT)
    imag_part = jnp.einsum(pattern, by_spin[1], anchor[0], precision=EXACT) - jnp.einsum(pattern, by_spin[0], anchor[1], precision=EXACT)
    return jnp.stack([real_part.reshape(SC * SC), imag_part.reshape(SC * SC)])


def sine_squares(length):
    wavenumber = jnp.arange(length, dtype=jnp.float32)
    return 4.0 * jnp.sin(math.pi * wavenumber / length) ** 2


def inverse_square():
    across = sine_squares(NX)
    sine_square = sine_squares(L)
    momentum = across[:, None, None] + sine_square[None, :, None] + sine_square[None, None, :]
    guarded = jnp.where(momentum > 0.0, momentum, 1.0)
    return jnp.where(momentum > 0.0, PEAK_SQUARE / guarded, 0.0)


def reference(links, propagator, sink_time, src_time, src_site):
    filter_weight = inverse_square()

    def fix_timeslice(lattice):
        overall = None
        for sweep_index in range(ITERS):
            divergence = jnp.roll(lattice[0], 1, axis=3) - lattice[0] + jnp.roll(lattice[1], L, axis=4) - lattice[1] + roll_depth(lattice[2], 1) - lattice[2]
            real_six, imag_six = project(divergence)
            packed = (real_six + 1j * imag_six).reshape(6, NX, L, L)
            spectrum = jnp.fft.fftn(packed, axes=(1, 2, 3)) * filter_weight[None]
            filtered = jnp.fft.ifftn(spectrum, axes=(1, 2, 3)).reshape(6, NX, L * L)
            algebra = assemble(jnp.real(filtered), jnp.imag(filtered))
            gauge_field = exponential(algebra * (STEP_SIZE / 16.0))
            lattice = rotate(lattice, gauge_field, jnp.roll(gauge_field, -1, axis=3))
            overall = gauge_field if overall is None else complex_product(gauge_field, overall)
        return lattice, overall

    fixed_links, overall_all = lax.map(fix_timeslice, links)
    sink_slice = sink_time[0] % NT
    source_slice = src_time[0] % NT
    wall_total = sink_product(overall_all[sink_slice], propagator)
    site_index = src_site[0]
    anchor = overall_all[source_slice][:, :, :, site_index // (L * L), site_index % (L * L)]
    wall = source_rotate(wall_total, anchor) * float(NX * L * L) ** -0.5
    return fixed_links, wall
```

```python
import functools
import math

import jax
import jax.numpy as jnp
import numpy as np
from jax import lax
from jax.experimental import pallas as pl
from jax.experimental.pallas import tpu as pltpu
from jax.sharding import PartitionSpec as P

SC = 12
ITERS = 2
STEP = 0.08 / 16.0
PEAK = 12.0
LANES = 128
FIELDS = 8
EXACT = lax.Precision.HIGHEST
MESH = pl.DeviceIdType.MESH
VMEM = pl.BlockSpec(memory_space=pltpu.VMEM)
SMEM = pl.BlockSpec(memory_space=pltpu.SMEM)
LIMIT = 60 * 1024 * 1024


def real_basis(n):
    x = np.arange(n)
    rows, moment = [], []
    for k in range(n // 2 + 1):
        angle = 2.0 * np.pi * ((k * x) % n) / n
        square = 4.0 * np.sin(np.pi * k / n) ** 2
        if k == 0 or 2 * k == n:
            rows.append(np.cos(angle) / np.sqrt(n))
            moment.append(square)
        else:
            rows.append(np.cos(angle) * np.sqrt(2.0 / n))
            rows.append(np.sin(angle) * np.sqrt(2.0 / n))
            moment += [square, square]
    return np.array(rows), np.array(moment)


def halves(m):
    high = m.astype(jnp.bfloat16)
    return high, (m - high.astype(np.float64)).astype(jnp.bfloat16)


def plane_matrices(q):
    n = q.shape[0]
    zero = np.zeros((n, n))
    right = np.block([[q.T, zero, zero, q.T], [zero, q.T, q.T, zero]])
    even, odd = q[0::2], q[1::2]
    left = np.block([[even[:, 0::2], even[:, 1::2]], [odd[:, 1::2], odd[:, 0::2]]])
    high, low = halves(right)
    right = np.concatenate([high, high, low], axis=0)
    high, low = halves(left)
    return right, np.concatenate([high, high, low], axis=1)


def triple(x, axis):
    high = x.astype(jnp.bfloat16)
    low = (x - high.astype(jnp.float32)).astype(jnp.bfloat16)
    return jnp.concatenate([high, low, high], axis=axis)


def dot(a, b):
    return jnp.dot(a, b, preferred_element_type=jnp.float32)


def plane_transform(slabs, right, left):
    rows = slabs[0].shape[0]
    wide = dot(triple(jnp.concatenate(slabs, axis=0), 1), right)
    count = len(slabs)
    straight = [wide[i * rows : (i + 1) * rows, :LANES] for i in range(count)]
    swapped = [wide[i * rows : (i + 1) * rows, LANES:] for i in range(count)]
    tall = jnp.concatenate(
        [jnp.concatenate(straight, axis=1), jnp.concatenate(swapped, axis=1)], axis=0
    )
    both = dot(left, triple(tall, 0))
    low = lax.broadcasted_iota(jnp.int32, (rows, LANES), 1) < LANES // 2
    return [
        jnp.where(
            low,
            both[:rows, i * LANES : (i + 1) * LANES],
            both[rows:, i * LANES : (i + 1) * LANES],
        )
        for i in range(count)
    ]


def lane_of(shape):
    return lax.broadcasted_iota(jnp.int32, shape, 1)


def y_behind(v):
    half = LANES // 2
    r = pltpu.roll(v, half, 1)
    return jnp.where(lane_of(v.shape) < half, pltpu.roll(r, 1, 0), r)


def y_ahead(v):
    half = LANES // 2
    r = pltpu.roll(v, half, 1)
    return jnp.where(lane_of(v.shape) < half, r, pltpu.roll(r, v.shape[0] - 1, 0))


def z_behind(v):
    half = LANES // 2
    edge = lane_of(v.shape) % half == 0
    return jnp.where(edge, pltpu.roll(v, half + 1, 1), pltpu.roll(v, 1, 1))


def z_ahead(v):
    half = LANES // 2
    edge = lane_of(v.shape) % half == half - 1
    return jnp.where(edge, pltpu.roll(v, half - 1, 1), pltpu.roll(v, LANES - 1, 1))


PAIRS = ((0, 1), (0, 2), (1, 2))


def project(get, f):
    if f < 6:
        a, b = PAIRS[f % 3]
        if f < 3:
            return 0.5 * (get(0, a, b) - get(0, b, a))
        return 0.5 * (get(1, a, b) + get(1, b, a))
    diag = [get(1, a, a) for a in range(3)]
    return diag[f - 6] - (diag[0] + diag[1] + diag[2]) * (1.0 / 3.0)


def cmul(a, b):
    return (a[0] * b[0] - a[1] * b[1], a[0] * b[1] + a[1] * b[0])


def exponential(fields):
    v = [STEP * f for f in fields]
    h0, h1 = v[6], v[7]
    h2 = -(h0 + h1)
    h01, h02, h12 = (v[3], -v[0]), (v[4], -v[1]), (v[5], -v[2])
    n01 = h01[0] * h01[0] + h01[1] * h01[1]
    n02 = h02[0] * h02[0] + h02[1] * h02[1]
    n12 = h12[0] * h12[0] + h12[1] * h12[1]
    c = 0.5 * (h0 * h0 + h1 * h1 + h2 * h2) + n01 + n02 + n12
    prod = cmul(h01, h12)
    triple = prod[0] * h02[0] + prod[1] * h02[1]
    d = h0 * h1 * h2 + 2.0 * triple - h0 * n12 - h1 * n02 - h2 * n01
    cd, cc, dd = c * d, c * c, d * d
    f0 = (1.0 - dd * (1 / 720), cd * (1 / 120) - d * (1 / 6))
    f1 = (d * (1 / 24) - cd * (1 / 360), 1.0 - c * (1 / 6) + cc * (1 / 120))
    f2 = (c * (1 / 24) - 0.5 - cc * (1 / 720), d * (1 / 120))
    for _ in range(3):
        s00, s01, s02 = cmul(f0, f0), cmul(f0, f1), cmul(f0, f2)
        s11, s12, s22 = cmul(f1, f1), cmul(f1, f2), cmul(f2, f2)
        f0 = tuple(s00[i] + 2.0 * d * s12[i] for i in range(2))
        f1 = tuple(2.0 * (s01[i] + c * s12[i]) + d * s22[i] for i in range(2))
        f2 = tuple(s11[i] + 2.0 * s02[i] + c * s22[i] for i in range(2))
    conj = lambda x: (x[0], -x[1])
    mixed = cmul(h02, conj(h12))
    q01 = (mixed[0] - h2 * h01[0], mixed[1] - h2 * h01[1])
    q02 = (prod[0] - h1 * h02[0], prod[1] - h1 * h02[1])
    mixed = cmul(conj(h01), h02)
    q12 = (mixed[0] - h0 * h12[0], mixed[1] - h0 * h12[1])
    diag = ((h0, h0 * h0 + n01 + n02), (h1, h1 * h1 + n01 + n12), (h2, h2 * h2 + n02 + n12))
    gauge = [[None] * 3 for _ in range(3)]
    for a in range(3):
        h, q = diag[a]
        gauge[a][a] = tuple(f0[i] + f1[i] * h + f2[i] * q for i in range(2))
    for a, b, h, q in ((0, 1, h01, q01), (0, 2, h02, q02), (1, 2, h12, q12)):
        x, y = cmul(f1, h), cmul(f2, q)
        gauge[a][b] = (x[0] + y[0], x[1] + y[1])
        x, y = cmul(f1, conj(h)), cmul(f2, conj(q))
        gauge[b][a] = (x[0] + y[0], x[1] + y[1])
    return gauge


def matmul3(left, right, adjoint=False):
    out = [[None] * 3 for _ in range(3)]
    for a in range(3):
        for b in range(3):
            re = im = None
            for k in range(3):
                xr, xi = left[a][k]
                yr, yi = right[b][k] if adjoint else right[k][b]
                if adjoint:
                    r, i = xr * yr + xi * yi, xi * yr - xr * yi
                else:
                    r, i = xr * yr - xi * yi, xr * yi + xi * yr
                re, im = (r, i) if re is None else (re + r, im + i)
            out[a][b] = (re, im)
    return out


def at(part, a, b):
    return part * 9 + a * 3 + b


class Swap:
    def __init__(self, size, send, recv, send_sem, recv_sem):
        self.size, self.send, self.recv = size, send, recv
        self.send_sem, self.recv_sem = send_sem, recv_sem
        self.me = lax.axis_index("space")

    def copy(self, g, off):
        peer = lax.rem(self.me + off, self.size)
        return pltpu.make_async_remote_copy(
            src_ref=self.send.at[g, peer],
            dst_ref=self.recv.at[g, self.me],
            send_sem=self.send_sem.at[g, off],
            recv_sem=self.recv_sem.at[g, off],
            device_id={"space": peer},
            device_id_type=MESH,
        )

    def start(self, g):
        for off in range(1, self.size):
            self.copy(g, off).start()
        self.recv[g, self.me] = self.send[g, self.me]

    def arrive(self, g):
        for off in range(1, self.size):
            self.copy(g, off).wait_recv()

    def drain(self):
        for g in range(self.send.shape[0]):
            for off in range(1, self.size):
                self.copy(g, off).wait_send()


class Relay:
    def __init__(self, size, root, own, up, down, sems):
        self.size, self.root, self.own = size, root, own
        self.up, self.down = up, down
        self.sems = sems
        self.me = lax.axis_index("tm")
        self.deep = min(size, 4)

    def hop(self, k, rise):
        buffer = self.up if rise else self.down
        base = 0 if rise else 2
        step = 1 if rise else self.size - 1
        return pltpu.make_async_remote_copy(
            src_ref=buffer.at[k],
            dst_ref=buffer.at[k],
            send_sem=self.sems.at[base, k],
            recv_sem=self.sems.at[base + 1, k],
            device_id={"tm": lax.rem(self.me + step, self.size)},
            device_id_type=MESH,
        )

    def step(self, k, h):
        for rise in (True, False):
            place = self.me if rise else self.size - 1 - self.me
            last = h == self.deep - 1
            here = (place >= h) if last else (place == h)
            buffer = self.up if rise else self.down
            parts = buffer.shape[1]

            @pl.when(here)
            def _():
                if h == 0:
                    for j in range(parts):
                        buffer[k, j] = self.own(k, j)
                else:
                    self.hop(k, rise).wait_recv()
                    mine = jnp.broadcast_to(self.root, buffer.shape[2:]) == self.me
                    for j in range(parts):
                        buffer[k, j] = jnp.where(mine, self.own(k, j), buffer[k, j])
                if not last:
                    self.hop(k, rise).start()
                elif self.size > self.deep:

                    @pl.when(place < self.size - 1)
                    def _():
                        self.hop(k, rise).start()

    def drain(self):
        for k in range(self.up.shape[0]):

            @pl.when(self.me < self.size - 1)
            def _():
                self.hop(k, True).wait_send()

            @pl.when(self.me > 0)
            def _():
                self.hop(k, False).wait_send()

    def value(self, k, j, band):
        own = self.own(k, j, band)
        root = jnp.broadcast_to(self.root, own.shape)
        other = jnp.where(root < self.me, self.up[k, j, band, :], self.down[k, j, band, :])
        return jnp.where(root == self.me, own, other)


def greet(axis, offsets, sizes):
    barrier = pltpu.get_barrier_semaphore()
    me = lax.axis_index(axis)
    for off in offsets:
        peer = lax.rem(me + off, sizes[axis])
        pl.semaphore_signal(barrier, inc=1, device_id={axis: peer}, device_id_type=MESH)
    return len(offsets)


class Plan:
    def __init__(self, sizes, planes, rows, basis, moment):
        self.sizes, self.planes, self.rows = sizes, planes, rows
        self.basis, self.moment = basis, moment
        self.size = sizes["space"]
        self.ratio = 8 * self.size // rows
        self.groups = FIELDS // self.ratio
        assert self.ratio * rows == 8 * self.size and self.groups * self.ratio == FIELDS
        self.levels = sorted(set(np.round(moment, 9)))
        self.chunk = (self.groups, self.size, planes + 1, 8, LANES)
        self.slab = (FIELDS * (planes + 1), rows, LANES)

    def fields(self, g):
        return range(g * self.ratio, (g + 1) * self.ratio)

    def exchange_scratch(self):
        sems = pltpu.SemaphoreType.DMA((self.groups, self.size))
        return [pltpu.VMEM(self.chunk, jnp.float32)] * 4 + [
            pltpu.VMEM((len(self.levels), 8, LANES), jnp.float32)
        ] + [sems] * 4


def weigh(plan, yz_ref, weight_ref):
    block = lax.div(lax.axis_index("space"), plan.ratio)
    yz = yz_ref[pl.ds(pl.multiple_of(block * 8, 8), 8), :]
    for index, level in enumerate(plan.levels):
        p2 = yz + float(level)
        if level == 0.0:
            weight = jnp.where(p2 > 0.0, PEAK / jnp.where(p2 > 0.0, p2, 1.0), 0.0)
        else:
            weight = PEAK / p2
        weight_ref[index] = weight


def forward(plan, u, g, right, left, send_ref):
    planes = plan.planes
    slabs = []
    for f in plan.fields(g):
        before = None
        for p in range(planes):
            x, y, z = (
                project(lambda part, a, b, i=i: u(i, part, a, b, p), f) for i in range(3)
            )
            value = (y_behind(y) - y + z_behind(z) - z) - x
            slabs.append(value if before is None else value + before)
            before = x
        slabs.append(before)
    done = plane_transform(slabs, right, left)
    for index, slab in enumerate(done):
        i, p = divmod(index, planes + 1)
        for block in range(plan.rows // 8):
            send_ref[g, block * plan.ratio + i, p] = slab[block * 8 : block * 8 + 8, :]


def backward(plan, g, right, left, recv_ref, slab_ref):
    slabs = []
    for i in range(plan.ratio):
        for p in range(plan.planes + 1):
            slabs.append(
                jnp.concatenate(
                    [recv_ref[g, b * plan.ratio + i, p] for b in range(plan.rows // 8)],
                    axis=0,
                )
            )
    base = g * plan.ratio * (plan.planes + 1)
    for index, slab in enumerate(plane_transform(slabs, right, left)):
        slab_ref[base + index] = slab


def across(plan, g, recv_ref, weight_ref, send_ref):
    planes, count, basis = plan.planes, plan.size, plan.basis
    n = basis.shape[0]
    v = []
    for s in range(count):
        for p in range(planes):
            value = recv_ref[g, s, p]
            if p == 0:
                value = value + recv_ref[g, (s - 1) % count, planes]
            v.append(value)
    half = range(1, (n + 1) // 2)
    even = {0: v[0]}
    odd = {}
    if n % 2 == 0:
        even[n // 2] = v[n // 2]
    for x in half:
        even[x] = v[x] + v[n - x]
        odd[x] = v[x] - v[n - x]
    back_even = {x: None for x in even}
    back_odd = {x: None for x in odd}
    for k in range(n):
        is_sine = abs(basis[k, 0]) < 1e-9
        source, target = (odd, back_odd) if is_sine else (even, back_even)
        mode = None
        for x in source:
            term = float(basis[k, x]) * source[x]
            mode = term if mode is None else mode + term
        mode = mode * weight_ref[plan.levels.index(np.round(plan.moment[k], 9))]
        for x in target:
            term = float(basis[k, x]) * mode
            target[x] = term if target[x] is None else target[x] + term
    out = [None] * n
    for x in back_even:
        out[x] = back_even[x]
    for x in half:
        out[x] = back_even[x] + back_odd[x]
        out[n - x] = back_even[x] - back_odd[x]
    for d in range(count):
        for p in range(planes + 1):
            send_ref[g, d, p] = out[(d * planes + p) % n]


def first_kernel(
    plan, links_ref, right_ref, left_ref, back_ref, turn_ref, yz_ref, slab_ref,
    send_one, recv_one, send_two, recv_two, weight_ref, *sems,
):
    planes, rows = plan.planes, plan.rows
    total = greet("space", range(1, plan.size), plan.sizes)
    one = Swap(plan.size, send_one, recv_one, sems[0], sems[1])
    two = Swap(plan.size, send_two, recv_two, sems[2], sems[3])

    def u(i, part, a, b, p):
        return links_ref[i * 18 + at(part, a, b), pl.ds(p, rows, planes), :]

    for g in range(plan.groups):
        forward(plan, u, g, right_ref[...], left_ref[...], send_one)
        if g == 0:
            pl.semaphore_wait(pltpu.get_barrier_semaphore(), total)
        one.start(g)
    weigh(plan, yz_ref, weight_ref)
    for g in range(plan.groups):
        one.arrive(g)
        across(plan, g, recv_one, weight_ref, send_two)
        two.start(g)
    for g in range(plan.groups):
        two.arrive(g)
        backward(plan, g, back_ref[...], turn_ref[...], recv_two, slab_ref)
    one.drain()
    two.drain()


def gauge_of(slab_ref, planes, gauge_ref):
    rows = gauge_ref.shape[2]

    for p in range(planes + 1):

        @pl.loop(0, rows // 8)
        def _(j):
            band = pl.ds(pl.multiple_of(j * 8, 8), 8)
            g = exponential([slab_ref[f * (planes + 1) + p, band, :] for f in range(FIELDS)])
            for a in range(3):
                for b in range(3):
                    for part in range(2):
                        gauge_ref[at(part, a, b), p, band, :] = g[a][b][part]


def shift_all(planes, gauge_ref, ahead_ref):
    for e in range(18):
        for p in range(planes):
            ahead_ref[e, p] = y_ahead(gauge_ref[e, p])
            ahead_ref[18 + e, p] = z_ahead(gauge_ref[e, p])


def rotate_plane(get_band, put_band, p, gauge_ref, ahead_ref):
    rows = gauge_ref.shape[2]

    @pl.loop(0, rows // 8)
    def _(j):
        start = pl.multiple_of(j * 8, 8)
        band = pl.ds(start, 8)
        for i in range(3):
            g = [
                [tuple(gauge_ref[at(r, a, b), p, band, :] for r in range(2)) for b in range(3)]
                for a in range(3)
            ]
            u = [
                [tuple(get_band(i, r, a, b, p, j) for r in range(2)) for b in range(3)]
                for a in range(3)
            ]
            if i == 0:
                source = lambda r, a, b: gauge_ref[at(r, a, b), p + 1, band, :]
            else:
                source = lambda r, a, b: ahead_ref[(i - 1) * 18 + at(r, a, b), p, band, :]
            ahead = [
                [tuple(source(r, a, b) for r in range(2)) for b in range(3)]
                for a in range(3)
            ]
            out = matmul3(matmul3(g, u), ahead, adjoint=True)
            for a in range(3):
                for b in range(3):
                    for r in range(2):
                        put_band(i, r, a, b, p, j, out[a][b][r])


def relay_order(chunks, deep):
    steps = [(k, h) for k in range(chunks) for h in range(1, deep)]
    return sorted(steps, key=lambda s: 1.4 * (s[0] + s[1]) + 2.1 * s[1])


def second_kernel(
    plan, root_ref, links_ref, slab_one, right_ref, left_ref, back_ref, turn_ref, yz_ref,
    out_ref, slab_two, spread_ref,
    send_one, recv_one, send_two, recv_two, weight_ref, sem_a, sem_b, sem_c, sem_d,
    gauge_ref, ahead_ref, up_ref, down_ref, relay_sems,
):
    planes, rows, sizes = plan.planes, plan.rows, plan.sizes
    total = greet("space", range(1, plan.size), sizes)
    total += greet("tm", (1, sizes["tm"] - 1), sizes)
    one = Swap(plan.size, send_one, recv_one, sem_a, sem_b)
    two = Swap(plan.size, send_two, recv_two, sem_c, sem_d)

    def own(k, j, band=slice(None)):
        i, p = divmod(j, planes)
        return slab_one[(k * plan.ratio + i) * (planes + 1) + p, band, :]

    relay = Relay(sizes["tm"], root_ref[0], own, up_ref, down_ref, relay_sems)
    gauge_of(slab_one, planes, gauge_ref)
    shift_all(planes, gauge_ref, ahead_ref)

    def get(i, r, a, b, p, j):
        return links_ref[i * 18 + at(r, a, b), pl.ds(j * 8 * planes + p, 8, planes), :]

    def put(i, r, a, b, p, j, value):
        out_ref[i * 18 + at(r, a, b), p, pl.ds(pl.multiple_of(j * 8, 8), 8), :] = value

    for p in range(planes):
        rotate_plane(get, put, p, gauge_ref, ahead_ref)

    def u(i, part, a, b, p):
        return out_ref[i * 18 + at(part, a, b), p]

    steps = relay_order(plan.groups, relay.deep)

    def advance(count):
        for _ in range(count):
            if steps:
                relay.step(*steps.pop(0))

    pl.semaphore_wait(pltpu.get_barrier_semaphore(), total)
    for k in range(plan.groups):
        relay.step(k, 0)
    for g in range(plan.groups):
        forward(plan, u, g, right_ref[...], left_ref[...], send_one)
        one.start(g)
    weigh(plan, yz_ref, weight_ref)
    advance(3)
    for g in range(plan.groups):
        one.arrive(g)
        across(plan, g, recv_one, weight_ref, send_two)
        two.start(g)
        advance(1)
    for g in range(plan.groups):
        advance(1)
        two.arrive(g)
        backward(plan, g, back_ref[...], turn_ref[...], recv_two, slab_two)
    advance(len(steps))
    for k in range(plan.groups):
        for j in range(plan.ratio * planes):
            i, p = divmod(j, planes)
            spread_ref[(k * plan.ratio + i) * planes + p] = relay.value(k, j, slice(None))
    one.drain()
    two.drain()
    relay.drain()


class Gather:
    def __init__(self, sizes, axes, target, send, recv):
        self.axes, self.target, self.send, self.recv = axes, target, send, recv
        me = [lax.axis_index(axis) for axis in axes]
        extent = [sizes[axis] for axis in axes]
        slot = 0
        for index, size in zip(me, extent):
            slot = slot * size + index
        self.slot = slot
        self.peers = []
        for flat in range(1, math.prod(extent)):
            rest, peer = flat, {}
            for axis, index, size in reversed(list(zip(axes, me, extent))):
                peer[axis] = lax.rem(index + rest % size, size)
                rest //= size
            self.peers.append((flat, peer))

    def greet(self):
        barrier = pltpu.get_barrier_semaphore()
        for _, peer in self.peers:
            pl.semaphore_signal(barrier, inc=1, device_id=peer, device_id_type=MESH)
        return len(self.peers)

    def run(self, source):
        copies = []
        for flat, peer in self.peers:
            copies.append(
                pltpu.make_async_remote_copy(
                    src_ref=source,
                    dst_ref=self.target.at[self.slot],
                    send_sem=self.send.at[flat],
                    recv_sem=self.recv.at[flat],
                    device_id=peer,
                    device_id_type=MESH,
                )
            )
            copies[-1].start()
        self.target[self.slot] = source[...]
        for copy in copies:
            copy.wait()


def third_kernel(
    plan, stages, scalar_ref, lattice_ref, slab_one, slab_two, spread_ref, prop_ref,
    out_ref, table_ref,
    gauge_ref, ahead_ref, up_ref, down_ref, relay_sems, acc_ref, sum_ref, row_ref, *gathers,
):
    planes, rows, sizes = plan.planes, plan.rows, plan.sizes
    root, present, plane, line, lane = (scalar_ref[i] for i in range(5))
    stages = [
        Gather(sizes, axes, *gathers[3 * i : 3 * i + 3]) for i, axes in enumerate(stages)
    ]
    total = sum(stage.greet() for stage in stages)

    def own(k, j, band=slice(None)):
        i, p = divmod(j, planes)
        return slab_two[(k * plan.ratio + i) * (planes + 1) + p, band, :]

    relay = Relay(sizes["tm"], root, own, up_ref, down_ref, relay_sems)
    pl.semaphore_wait(pltpu.get_barrier_semaphore(), total)
    for k in range(plan.groups):
        relay.step(k, 0)
    steps = relay_order(plan.groups, relay.deep)

    def advance(count):
        for _ in range(count):
            if steps:
                relay.step(*steps.pop(0))

    gauge_of(slab_two, planes, gauge_ref)
    shift_all(planes, gauge_ref, ahead_ref)

    def get(i, r, a, b, p, j):
        return lattice_ref[i * 18 + at(r, a, b), p, pl.ds(pl.multiple_of(j * 8, 8), 8), :]

    def put(i, r, a, b, p, j, value):
        out_ref[i * 18 + at(r, a, b), pl.ds(j * 8 * planes + p, 8, planes), :] = value

    for p in range(planes):
        rotate_plane(get, put, p, gauge_ref, ahead_ref)
        advance(2)
    acc_ref[...] = jnp.zeros_like(acc_ref)
    sum_ref[...] = jnp.zeros_like(sum_ref)
    spot = (lax.broadcasted_iota(jnp.int32, (rows, LANES), 0) == line) & (
        lax.broadcasted_iota(jnp.int32, (rows, LANES), 1) == lane
    )

    def pick(ref, f):
        value = jnp.zeros((1, 1), jnp.float32)
        for p in range(planes):
            here = spot & (plane == p)
            entry = ref[f * (planes + 1) + p]
            value = value + jnp.sum(jnp.where(here, entry, 0.0), keepdims=True)
        return jnp.broadcast_to(value, (8, LANES))

    anchor = matmul3(
        exponential([pick(slab_two, f) for f in range(FIELDS)]),
        exponential([pick(slab_one, f) for f in range(FIELDS)]),
    )
    pairs = prop_ref.shape[0] // 2
    first = lane_of((1, LANES)) == 0
    for r in range(2):
        for a in range(3):
            for b in range(3):
                e = 2 * pairs + at(r, a, b)
                sum_ref[e : e + 1, :] = jnp.where(
                    first & (present > 0), anchor[a][b][r][0:1, :], 0.0
                )
    advance(len(steps))

    for p in range(planes):

        @pl.loop(0, rows // 8)
        def _(j):
            band = pl.ds(pl.multiple_of(j * 8, 8), 8)
            one = exponential([spread_ref[f * planes + p, band, :] for f in range(FIELDS)])
            two = exponential(
                [
                    relay.value(f // plan.ratio, (f % plan.ratio) * planes + p, band)
                    for f in range(FIELDS)
                ]
            )
            t = matmul3(two, one)
            for q in range(pairs // 3):
                s = [
                    tuple(
                        prop_ref[r * pairs + q * 3 + k, pl.ds(j * 8 * planes + p, 8, planes), :]
                        for r in range(2)
                    )
                    for k in range(3)
                ]
                for a in range(3):
                    re = im = None
                    for k in range(3):
                        x = cmul(t[a][k], s[k])
                        re, im = x if re is None else (re + x[0], im + x[1])
                    acc_ref[q * 3 + a] += re
                    acc_ref[pairs + q * 3 + a] += im

    for e in range(2 * pairs):
        sum_ref[e : e + 1, :] = jnp.sum(acc_ref[e], axis=0, keepdims=True)
    row_ref[...] = lax.dot_general(
        jnp.ones((8, LANES), jnp.float32),
        sum_ref[...],
        (((1,), (1,)), ((), ())),
        precision=EXACT,
        preferred_element_type=jnp.float32,
    )[0:1, :]
    space, times = sizes["space"], sizes["tm"]
    stages[0].run(row_ref)
    if len(stages) == 1:
        for t in range(times):
            value = stages[0].target[t]
            for s in range(1, space):
                value = value + stages[0].target[s * times + t]
            table_ref[t : t + 1, :] = value
    else:
        value = stages[0].target[0]
        for s in range(1, space):
            value = value + stages[0].target[s]
        row_ref[...] = value
        stages[1].run(row_ref)
        for t in range(times):
            table_ref[t : t + 1, :] = stages[1].target[t]
    relay.drain()


def call(kernel, outs, scratch, args, collective_id, smem=0):
    return pl.pallas_call(
        kernel,
        out_shape=[jax.ShapeDtypeStruct(s, jnp.float32) for s in outs],
        in_specs=[SMEM] * smem + [VMEM] * (len(args) - smem),
        out_specs=[VMEM] * len(outs),
        scratch_shapes=[
            pltpu.VMEM(s, jnp.float32) if isinstance(s, tuple) else s for s in scratch
        ],
        compiler_params=pltpu.CompilerParams(
            collective_id=collective_id, has_side_effects=True, vmem_limit_bytes=LIMIT
        ),
    )(*args)


def body(sizes, links, propagator, sink_time, src_time, src_site):
    space, times = sizes["space"], sizes["tm"]
    planes, area = links.shape[5], links.shape[6]
    side = math.isqrt(area)
    wide = planes * space
    rows = area // LANES
    assert side * 2 == LANES and rows % 8 == 0

    basis, moment = real_basis(side)
    right, left = plane_matrices(basis)
    back, turn = plane_matrices(basis.T)
    x_basis, x_moment = real_basis(wide)
    yz = (moment.reshape(rows, 2, 1) + moment[None, None, :]).reshape(rows, LANES)
    yz = yz.astype(np.float32)
    plan = Plan(sizes, planes, rows, x_basis, x_moment)

    def fold(x):
        lead = x.shape[:-2]
        x = x.reshape(lead + (planes, rows, LANES))
        return jnp.swapaxes(x, -3, -2).reshape((-1, rows * planes, LANES))

    linked = fold(links[0])
    field = (FIELDS * planes, rows, LANES)
    gauge = (18, planes + 1, rows, LANES)
    ahead = (36, planes, rows, LANES)
    split = (54, planes, rows, LANES)
    spread = (plan.groups, plan.ratio * planes, rows, LANES)
    relay_sems = pltpu.SemaphoreType.DMA((4, plan.groups))

    site = src_site[0]
    space_index = lax.axis_index("space")
    time_index = lax.axis_index("tm")
    plane = site // area - space_index * planes
    column = site % area
    present = (src_time[0] % times == time_index) & (plane >= 0) & (plane < planes)
    scalars = jnp.stack(
        [
            sink_time[0] % times,
            present.astype(jnp.int32),
            plane,
            column // LANES,
            column % LANES,
        ]
    )

    (slab_one,) = call(
        functools.partial(first_kernel, plan),
        [plan.slab],
        plan.exchange_scratch(),
        [linked, right, left, back, turn, yz],
        0,
    )
    lattice, slab_two, spread_one = call(
        functools.partial(second_kernel, plan),
        [split, plan.slab, field],
        plan.exchange_scratch() + [gauge, ahead, spread, spread, relay_sems],
        [scalars, linked, slab_one, right, left, back, turn, yz],
        1,
        smem=1,
    )
    pairs = propagator.shape[1]
    assert 2 * pairs + 18 <= LANES
    stages = [("space", "tm")] if space * times <= 64 else [("space",), ("tm",)]
    gathers = []
    for axes in stages:
        count = math.prod(sizes[axis] for axis in axes)
        gathers += [(count, 1, LANES)] + [pltpu.SemaphoreType.DMA((count,))] * 2
    final, table = call(
        functools.partial(third_kernel, plan, stages),
        [(54, rows * planes, LANES), (times, LANES)],
        [gauge, ahead, spread, spread, relay_sems]
        + [(2 * pairs, 8, LANES), (LANES, LANES), (1, LANES)]
        + gathers,
        [scalars, lattice, slab_one, slab_two, spread_one, fold(propagator)],
        2,
        smem=1,
    )
    final = jnp.swapaxes(final.reshape(54, rows, planes, LANES), 1, 2)
    final = final.reshape(links.shape)
    summed = table[:, : 2 * pairs].reshape(times, 2, pairs)
    summed = jnp.swapaxes(summed, 0, 1).reshape(2, 4, 3, SC)
    anchor = jnp.sum(table[:, 2 * pairs : 2 * pairs + 18], axis=0).reshape(2, 3, 3)
    left_re, left_im = summed[0][:, None], summed[1][:, None]
    right_re, right_im = (anchor[i][None, :, :, None] for i in range(2))
    real = jnp.sum(left_re * right_re + left_im * right_im, axis=2)
    imag = jnp.sum(left_im * right_re - left_re * right_im, axis=2)
    wall = jnp.stack([real.reshape(SC * SC), imag.reshape(SC * SC)])
    return final, wall * float(wide * area) ** (-0.5)


def solution(mesh):
    sizes = {axis: mesh.shape[axis] for axis in ("space", "tm")}
    placed = (
        P("tm", None, None, None, None, "space", None),
        P(None, "tm", "space", None),
        P(),
        P(),
        P(),
    )
    return jax.shard_map(
        functools.partial(body, sizes),
        mesh=mesh,
        in_specs=placed,
        out_specs=(P("tm", None, None, None, None, "space", None), P()),
        check_vma=False,
    )
```

```python
import functools
import math

import jax
import jax.numpy as jnp
import numpy as np
from jax import lax
from jax.experimental import pallas as pl
from jax.experimental.pallas import tpu as pltpu
from jax.sharding import PartitionSpec as P

SC = 12
ITERS = 2
STEP = 0.08 / 16.0
PEAK = 12.0
LANES = 128
FIELDS = 8
EXACT = lax.Precision.HIGHEST
MESH = pl.DeviceIdType.MESH
VMEM = pl.BlockSpec(memory_space=pltpu.VMEM)
SMEM = pl.BlockSpec(memory_space=pltpu.SMEM)
ANY = pl.BlockSpec(memory_space=pl.ANY)
LIMIT = 60 * 1024 * 1024


def real_basis(n):
    x = np.arange(n)
    rows, moment = [], []
    for k in range(n // 2 + 1):
        angle = 2.0 * np.pi * ((k * x) % n) / n
        square = 4.0 * np.sin(np.pi * k / n) ** 2
        if k == 0 or 2 * k == n:
            rows.append(np.cos(angle) / np.sqrt(n))
            moment.append(square)
        else:
            rows.append(np.cos(angle) * np.sqrt(2.0 / n))
            rows.append(np.sin(angle) * np.sqrt(2.0 / n))
            moment += [square, square]
    return np.array(rows), np.array(moment)


def halves(m):
    high = m.astype(jnp.bfloat16)
    return high, (m - high.astype(np.float64)).astype(jnp.bfloat16)


def plane_matrices(q):
    n = q.shape[0]
    zero = np.zeros((n, n))
    right = np.block([[q.T, zero, zero, q.T], [zero, q.T, q.T, zero]])
    even, odd = q[0::2], q[1::2]
    left = np.block([[even[:, 0::2], even[:, 1::2]], [odd[:, 1::2], odd[:, 0::2]]])
    high, low = halves(right)
    right = np.concatenate([high, high, low], axis=0)
    high, low = halves(left)
    return right, np.concatenate([high, high, low], axis=1)


def triple(x, axis):
    high = x.astype(jnp.bfloat16)
    low = (x - high.astype(jnp.float32)).astype(jnp.bfloat16)
    return jnp.concatenate([high, low, high], axis=axis)


def dot(a, b):
    return jnp.dot(a, b, preferred_element_type=jnp.float32)


def plane_transform(slabs, right, left):
    rows = slabs[0].shape[0]
    wide = dot(triple(jnp.concatenate(slabs, axis=0), 1), right)
    count = len(slabs)
    straight = [wide[i * rows : (i + 1) * rows, :LANES] for i in range(count)]
    swapped = [wide[i * rows : (i + 1) * rows, LANES:] for i in range(count)]
    tall = jnp.concatenate(
        [jnp.concatenate(straight, axis=1), jnp.concatenate(swapped, axis=1)], axis=0
    )
    both = dot(left, triple(tall, 0))
    low = lax.broadcasted_iota(jnp.int32, (rows, LANES), 1) < LANES // 2
    return [
        jnp.where(
            low,
            both[:rows, i * LANES : (i + 1) * LANES],
            both[rows:, i * LANES : (i + 1) * LANES],
        )
        for i in range(count)
    ]


def lane_of(shape):
    return lax.broadcasted_iota(jnp.int32, shape, 1)


def y_behind(v):
    half = LANES // 2
    r = pltpu.roll(v, half, 1)
    return jnp.where(lane_of(v.shape) < half, pltpu.roll(r, 1, 0), r)


def y_ahead(v):
    half = LANES // 2
    r = pltpu.roll(v, half, 1)
    return jnp.where(lane_of(v.shape) < half, r, pltpu.roll(r, v.shape[0] - 1, 0))


def z_behind(v):
    half = LANES // 2
    edge = lane_of(v.shape) % half == 0
    return jnp.where(edge, pltpu.roll(v, half + 1, 1), pltpu.roll(v, 1, 1))


def z_ahead(v):
    half = LANES // 2
    edge = lane_of(v.shape) % half == half - 1
    return jnp.where(edge, pltpu.roll(v, half - 1, 1), pltpu.roll(v, LANES - 1, 1))


PAIRS = ((0, 1), (0, 2), (1, 2))


def project(get, f):
    if f < 6:
        a, b = PAIRS[f % 3]
        if f < 3:
            return 0.5 * (get(0, a, b) - get(0, b, a))
        return 0.5 * (get(1, a, b) + get(1, b, a))
    diag = [get(1, a, a) for a in range(3)]
    return diag[f - 6] - (diag[0] + diag[1] + diag[2]) * (1.0 / 3.0)


def cmul(a, b):
    return (a[0] * b[0] - a[1] * b[1], a[0] * b[1] + a[1] * b[0])


def exponential(fields):
    v = [STEP * f for f in fields]
    h0, h1 = v[6], v[7]
    h2 = -(h0 + h1)
    h01, h02, h12 = (v[3], -v[0]), (v[4], -v[1]), (v[5], -v[2])
    n01 = h01[0] * h01[0] + h01[1] * h01[1]
    n02 = h02[0] * h02[0] + h02[1] * h02[1]
    n12 = h12[0] * h12[0] + h12[1] * h12[1]
    c = 0.5 * (h0 * h0 + h1 * h1 + h2 * h2) + n01 + n02 + n12
    prod = cmul(h01, h12)
    triple = prod[0] * h02[0] + prod[1] * h02[1]
    d = h0 * h1 * h2 + 2.0 * triple - h0 * n12 - h1 * n02 - h2 * n01
    cd, cc, dd = c * d, c * c, d * d
    f0 = (1.0 - dd * (1 / 720), cd * (1 / 120) - d * (1 / 6))
    f1 = (d * (1 / 24) - cd * (1 / 360), 1.0 - c * (1 / 6) + cc * (1 / 120))
    f2 = (c * (1 / 24) - 0.5 - cc * (1 / 720), d * (1 / 120))
    for _ in range(3):
        s00, s01, s02 = cmul(f0, f0), cmul(f0, f1), cmul(f0, f2)
        s11, s12, s22 = cmul(f1, f1), cmul(f1, f2), cmul(f2, f2)
        f0 = tuple(s00[i] + 2.0 * d * s12[i] for i in range(2))
        f1 = tuple(2.0 * (s01[i] + c * s12[i]) + d * s22[i] for i in range(2))
        f2 = tuple(s11[i] + 2.0 * s02[i] + c * s22[i] for i in range(2))
    conj = lambda x: (x[0], -x[1])
    mixed = cmul(h02, conj(h12))
    q01 = (mixed[0] - h2 * h01[0], mixed[1] - h2 * h01[1])
    q02 = (prod[0] - h1 * h02[0], prod[1] - h1 * h02[1])
    mixed = cmul(conj(h01), h02)
    q12 = (mixed[0] - h0 * h12[0], mixed[1] - h0 * h12[1])
    diag = ((h0, h0 * h0 + n01 + n02), (h1, h1 * h1 + n01 + n12), (h2, h2 * h2 + n02 + n12))
    gauge = [[None] * 3 for _ in range(3)]
    for a in range(3):
        h, q = diag[a]
        gauge[a][a] = tuple(f0[i] + f1[i] * h + f2[i] * q for i in range(2))
    for a, b, h, q in ((0, 1, h01, q01), (0, 2, h02, q02), (1, 2, h12, q12)):
        x, y = cmul(f1, h), cmul(f2, q)
        gauge[a][b] = (x[0] + y[0], x[1] + y[1])
        x, y = cmul(f1, conj(h)), cmul(f2, conj(q))
        gauge[b][a] = (x[0] + y[0], x[1] + y[1])
    return gauge


def matmul3(left, right, adjoint=False):
    out = [[None] * 3 for _ in range(3)]
    for a in range(3):
        for b in range(3):
            re = im = None
            for k in range(3):
                xr, xi = left[a][k]
                yr, yi = right[b][k] if adjoint else right[k][b]
                if adjoint:
                    r, i = xr * yr + xi * yi, xi * yr - xr * yi
                else:
                    r, i = xr * yr - xi * yi, xr * yi + xi * yr
                re, im = (r, i) if re is None else (re + r, im + i)
            out[a][b] = (re, im)
    return out


def at(part, a, b):
    return part * 9 + a * 3 + b


class Swap:
    def __init__(self, size, send, recv, send_sem, recv_sem):
        self.size, self.send, self.recv = size, send, recv
        self.send_sem, self.recv_sem = send_sem, recv_sem
        self.me = lax.axis_index("space")

    def copy(self, g, off):
        peer = lax.rem(self.me + off, self.size)
        return pltpu.make_async_remote_copy(
            src_ref=self.send.at[g, peer],
            dst_ref=self.recv.at[g, self.me],
            send_sem=self.send_sem.at[g, off],
            recv_sem=self.recv_sem.at[g, off],
            device_id={"space": peer},
            device_id_type=MESH,
        )

    def start(self, g):
        for off in range(1, self.size):
            self.copy(g, off).start()
        self.recv[g, self.me] = self.send[g, self.me]

    def arrive(self, g):
        for off in range(1, self.size):
            self.copy(g, off).wait_recv()

    def drain(self):
        for g in range(self.send.shape[0]):
            for off in range(1, self.size):
                self.copy(g, off).wait_send()


class Relay:
    def __init__(self, size, root, own, up, down, sems):
        self.size, self.root, self.own = size, root, own
        self.up, self.down = up, down
        self.sems = sems
        self.me = lax.axis_index("tm")
        self.deep = min(size, 4)

    def hop(self, k, rise):
        buffer = self.up if rise else self.down
        base = 0 if rise else 2
        step = 1 if rise else self.size - 1
        return pltpu.make_async_remote_copy(
            src_ref=buffer.at[k],
            dst_ref=buffer.at[k],
            send_sem=self.sems.at[base, k],
            recv_sem=self.sems.at[base + 1, k],
            device_id={"tm": lax.rem(self.me + step, self.size)},
            device_id_type=MESH,
        )

    def step(self, k, h):
        for rise in (True, False):
            place = self.me if rise else self.size - 1 - self.me
            last = h == self.deep - 1
            here = (place >= h) if last else (place == h)
            buffer = self.up if rise else self.down
            parts = buffer.shape[1]

            @pl.when(here)
            def _():
                if h == 0:
                    for j in range(parts):
                        buffer[k, j] = self.own(k, j)
                else:
                    self.hop(k, rise).wait_recv()
                    mine = jnp.broadcast_to(self.root, buffer.shape[2:]) == self.me
                    for j in range(parts):
                        buffer[k, j] = jnp.where(mine, self.own(k, j), buffer[k, j])
                if not last:
                    self.hop(k, rise).start()
                elif self.size > self.deep:

                    @pl.when(place < self.size - 1)
                    def _():
                        self.hop(k, rise).start()

    def drain(self):
        for k in range(self.up.shape[0]):

            @pl.when(self.me < self.size - 1)
            def _():
                self.hop(k, True).wait_send()

            @pl.when(self.me > 0)
            def _():
                self.hop(k, False).wait_send()

    def value(self, k, j, band):
        own = self.own(k, j, band)
        root = jnp.broadcast_to(self.root, own.shape)
        other = jnp.where(root < self.me, self.up[k, j, band, :], self.down[k, j, band, :])
        return jnp.where(root == self.me, own, other)


class Plan:
    def __init__(self, sizes, planes, rows, basis, moment):
        self.sizes, self.planes, self.rows = sizes, planes, rows
        self.basis, self.moment = basis, moment
        self.size = sizes["space"]
        self.ratio = 8 * self.size // rows
        self.groups = FIELDS // self.ratio
        assert self.ratio * rows == 8 * self.size and self.groups * self.ratio == FIELDS
        self.levels = sorted(set(np.round(moment, 9)))
        self.chunk = (self.groups, self.size, planes + 1, 8, LANES)
        self.slab = (FIELDS * (planes + 1), rows, LANES)

    def fields(self, g):
        return range(g * self.ratio, (g + 1) * self.ratio)


def weigh(plan, yz_ref, weight_ref):
    block = lax.div(lax.axis_index("space"), plan.ratio)
    yz = yz_ref[pl.ds(pl.multiple_of(block * 8, 8), 8), :]
    for index, level in enumerate(plan.levels):
        p2 = yz + float(level)
        if level == 0.0:
            weight = jnp.where(p2 > 0.0, PEAK / jnp.where(p2 > 0.0, p2, 1.0), 0.0)
        else:
            weight = PEAK / p2
        weight_ref[index] = weight


def forward(plan, u, g, right, left, send_ref):
    planes = plan.planes
    slabs = []
    for f in plan.fields(g):
        before = None
        for p in range(planes):
            x, y, z = (
                project(lambda part, a, b, i=i: u(i, part, a, b, p), f) for i in range(3)
            )
            value = (y_behind(y) - y + z_behind(z) - z) - x
            slabs.append(value if before is None else value + before)
            before = x
        slabs.append(before)
    done = plane_transform(slabs, right, left)
    for index, slab in enumerate(done):
        i, p = divmod(index, planes + 1)
        for block in range(plan.rows // 8):
            send_ref[g, block * plan.ratio + i, p] = slab[block * 8 : block * 8 + 8, :]


def backward(plan, g, right, left, recv_ref, slab_ref):
    slabs = []
    for i in range(plan.ratio):
        for p in range(plan.planes + 1):
            slabs.append(
                jnp.concatenate(
                    [recv_ref[g, b * plan.ratio + i, p] for b in range(plan.rows // 8)],
                    axis=0,
                )
            )
    base = g * plan.ratio * (plan.planes + 1)
    for index, slab in enumerate(plane_transform(slabs, right, left)):
        slab_ref[base + index] = slab


def across(plan, g, recv_ref, weight_ref, send_ref):
    planes, count, basis = plan.planes, plan.size, plan.basis
    n = basis.shape[0]
    v = []
    for s in range(count):
        for p in range(planes):
            value = recv_ref[g, s, p]
            if p == 0:
                value = value + recv_ref[g, (s - 1) % count, planes]
            v.append(value)
    half = range(1, (n + 1) // 2)
    even = {0: v[0]}
    odd = {}
    if n % 2 == 0:
        even[n // 2] = v[n // 2]
    for x in half:
        even[x] = v[x] + v[n - x]
        odd[x] = v[x] - v[n - x]
    back_even = {x: None for x in even}
    back_odd = {x: None for x in odd}
    for k in range(n):
        is_sine = abs(basis[k, 0]) < 1e-9
        source, target = (odd, back_odd) if is_sine else (even, back_even)
        mode = None
        for x in source:
            term = float(basis[k, x]) * source[x]
            mode = term if mode is None else mode + term
        mode = mode * weight_ref[plan.levels.index(np.round(plan.moment[k], 9))]
        for x in target:
            term = float(basis[k, x]) * mode
            target[x] = term if target[x] is None else target[x] + term
    out = [None] * n
    for x in back_even:
        out[x] = back_even[x]
    for x in half:
        out[x] = back_even[x] + back_odd[x]
        out[n - x] = back_even[x] - back_odd[x]
    for d in range(count):
        for p in range(planes + 1):
            send_ref[g, d, p] = out[(d * planes + p) % n]


def gauge_of(slab_ref, planes, gauge_ref):
    rows = gauge_ref.shape[2]

    for p in range(planes + 1):

        @pl.loop(0, rows // 8)
        def _(j):
            band = pl.ds(pl.multiple_of(j * 8, 8), 8)
            g = exponential([slab_ref[f * (planes + 1) + p, band, :] for f in range(FIELDS)])
            for a in range(3):
                for b in range(3):
                    for part in range(2):
                        gauge_ref[at(part, a, b), p, band, :] = g[a][b][part]


def shift_all(planes, gauge_ref, ahead_ref):
    for e in range(18):
        for p in range(planes):
            ahead_ref[e, p] = y_ahead(gauge_ref[e, p])
            ahead_ref[18 + e, p] = z_ahead(gauge_ref[e, p])


def rotate_plane(get_band, put_band, p, gauge_ref, ahead_ref):
    rows = gauge_ref.shape[2]

    @pl.loop(0, rows // 8)
    def _(j):
        start = pl.multiple_of(j * 8, 8)
        band = pl.ds(start, 8)
        for i in range(3):
            g = [
                [tuple(gauge_ref[at(r, a, b), p, band, :] for r in range(2)) for b in range(3)]
                for a in range(3)
            ]
            u = [
                [tuple(get_band(i, r, a, b, p, j) for r in range(2)) for b in range(3)]
                for a in range(3)
            ]
            if i == 0:
                source = lambda r, a, b: gauge_ref[at(r, a, b), p + 1, band, :]
            else:
                source = lambda r, a, b: ahead_ref[(i - 1) * 18 + at(r, a, b), p, band, :]
            ahead = [
                [tuple(source(r, a, b) for r in range(2)) for b in range(3)]
                for a in range(3)
            ]
            out = matmul3(matmul3(g, u), ahead, adjoint=True)
            for a in range(3):
                for b in range(3):
                    for r in range(2):
                        put_band(i, r, a, b, p, j, out[a][b][r])


class Steps:
    def __init__(self, relay, start):
        self.relay, self.start = relay, start
        chunks = relay.up.shape[0]
        self.left = sorted(
            [(k, h) for k in range(chunks) for h in range(1, relay.deep)], key=self.ready
        )

    def ready(self, step):
        return self.start + 0.7 * step[0] + 2.8 * step[1]

    def until(self, time, keep=0):
        while len(self.left) > keep and self.ready(self.left[0]) <= time:
            self.relay.step(*self.left.pop(0))


class Gather:
    def __init__(self, sizes, axes, target, send, recv):
        self.axes, self.target, self.send, self.recv = axes, target, send, recv
        me = [lax.axis_index(axis) for axis in axes]
        extent = [sizes[axis] for axis in axes]
        slot = 0
        for index, size in zip(me, extent):
            slot = slot * size + index
        self.slot = slot
        self.peers = []
        for flat in range(1, math.prod(extent)):
            rest, peer = flat, {}
            for axis, index, size in reversed(list(zip(axes, me, extent))):
                peer[axis] = lax.rem(index + rest % size, size)
                rest //= size
            self.peers.append((flat, peer))

    def greet(self):
        barrier = pltpu.get_barrier_semaphore()
        for _, peer in self.peers:
            pl.semaphore_signal(barrier, inc=1, device_id=peer, device_id_type=MESH)
        return len(self.peers)

    def run(self, source):
        copies = []
        for flat, peer in self.peers:
            copies.append(
                pltpu.make_async_remote_copy(
                    src_ref=source,
                    dst_ref=self.target.at[self.slot],
                    send_sem=self.send.at[flat],
                    recv_sem=self.recv.at[flat],
                    device_id=peer,
                    device_id_type=MESH,
                )
            )
            copies[-1].start()
        self.target[self.slot] = source[...]
        for copy in copies:
            copy.wait()


def main_kernel(
    plan, stages, sink_ref, src_ref, site_ref, links_any, right_any, left_any, back_any,
    turn_any, yz_any, prop_any,
    out_ref, table_ref,
    links_ref, right_ref, left_ref, back_ref, turn_ref, yz_ref, prop_ref, load_sems,
    send_ref, recv_ref, swap_sems, weight_ref, slab_one, slab_two, lattice_ref,
    gauge_ref, ahead_ref, up_ref, down_ref, relay_sems, acc_ref, sum_ref, row_ref, *gathers,
):
    planes, rows, sizes = plan.planes, plan.rows, plan.sizes
    space, times = sizes["space"], sizes["tm"]
    stages = [
        Gather(sizes, axes, *gathers[3 * i : 3 * i + 3]) for i, axes in enumerate(stages)
    ]
    total = sum(stage.greet() for stage in stages)

    pairs_of = [
        (right_any, right_ref), (left_any, left_ref), (back_any, back_ref),
        (turn_any, turn_ref), (yz_any, yz_ref), (prop_any, prop_ref),
    ]
    early = [
        pltpu.make_async_copy(
            links_any.at[pl.ds(i * 18, 18)], links_ref.at[pl.ds(i * 18, 18)], load_sems.at[i]
        )
        for i in range(3)
    ]
    late = [
        pltpu.make_async_copy(a, b, load_sems.at[3 + i]) for i, (a, b) in enumerate(pairs_of)
    ]
    early += late[:2]
    late = late[2:]
    for copy in early + late:
        copy.start()

    swaps = [
        Swap(space, send_ref.at[i], recv_ref.at[i], swap_sems.at[2 * i], swap_sems.at[2 * i + 1])
        for i in range(2 * ITERS)
    ]
    root = lax.rem(sink_ref[0], times)

    def owner(slab):
        def own(k, j, band=slice(None)):
            g, p = divmod(k, planes)
            return slab[(g * plan.ratio + j) * (planes + 1) + p, band, :]

        return own

    relays = [
        Relay(times, root, owner(slab), up_ref.at[i], down_ref.at[i], relay_sems.at[i])
        for i, slab in enumerate((slab_one, slab_two))
    ]
    steps = [Steps(relay, 0.8) for relay in relays]

    def sweep(u, index, before=lambda: None):
        one, two = swaps[2 * index], swaps[2 * index + 1]
        slab, relay = (slab_one, slab_two)[index], relays[index]
        for g in range(plan.groups):
            forward(plan, u, g, right_ref[...], left_ref[...], one.send)
            if g == 0:
                before()
            one.start(g)
            if index:
                steps[0].until(6.5 + 0.3 * g)
        if index == 0:
            for copy in late[:3]:
                copy.wait()
            weigh(plan, yz_ref, weight_ref)
        for g in range(plan.groups):
            if index:
                steps[0].until(10.6 + 1.05 * g)
            one.arrive(g)
            across(plan, g, one.recv, weight_ref, two.send)
            two.start(g)
        if index:
            steps[0].until(1e9)
        for g in range(plan.groups):
            two.arrive(g)
            backward(plan, g, back_ref[...], turn_ref[...], two.recv, slab)
            for p in range(planes):
                relay.step(g * planes + p, 0)

    for copy in early:
        copy.wait()

    def first(i, part, a, b, p):
        return links_ref[i * 18 + at(part, a, b), pl.ds(p, rows, planes), :]

    sweep(first, 0, lambda: pl.semaphore_wait(pltpu.get_barrier_semaphore(), total))
    steps[0].until(3.6)
    gauge_of(slab_one, planes, gauge_ref)
    steps[0].until(4.3)
    shift_all(planes, gauge_ref, ahead_ref)

    def get(i, r, a, b, p, j):
        return links_ref[i * 18 + at(r, a, b), pl.ds(j * 8 * planes + p, 8, planes), :]

    def put(i, r, a, b, p, j, value):
        lattice_ref[i * 18 + at(r, a, b), p, pl.ds(pl.multiple_of(j * 8, 8), 8), :] = value

    for p in range(planes):
        rotate_plane(get, put, p, gauge_ref, ahead_ref)
        steps[0].until(5.3 + 0.7 * p)

    sweep(lambda i, part, a, b, p: lattice_ref[i * 18 + at(part, a, b), p], 1)

    time = [3.6]

    def pause(length):
        time[0] += length
        steps[1].until(time[0])

    pause(0.0)
    gauge_of(slab_two, planes, gauge_ref)
    pause(0.7)
    shift_all(planes, gauge_ref, ahead_ref)
    pause(0.4)

    def get_last(i, r, a, b, p, j):
        return lattice_ref[i * 18 + at(r, a, b), p, pl.ds(pl.multiple_of(j * 8, 8), 8), :]

    def put_last(i, r, a, b, p, j, value):
        out_ref[i * 18 + at(r, a, b), pl.ds(j * 8 * planes + p, 8, planes), :] = value

    for p in range(planes):
        rotate_plane(get_last, put_last, p, gauge_ref, ahead_ref)
        pause(0.7)
    for p in range(planes):

        @pl.loop(0, rows // 8)
        def _(j):
            band = pl.ds(pl.multiple_of(j * 8, 8), 8)
            one = exponential(
                [
                    relays[0].value((f // plan.ratio) * planes + p, f % plan.ratio, band)
                    for f in range(FIELDS)
                ]
            )
            for a in range(3):
                for b in range(3):
                    for part in range(2):
                        ahead_ref[at(part, a, b), p, band, :] = one[a][b][part]

    pause(0.6)
    acc_ref[...] = jnp.zeros_like(acc_ref)
    sum_ref[...] = jnp.zeros_like(sum_ref)
    site = site_ref[0]
    column = lax.rem(site, rows * LANES)
    plane = lax.div(site, rows * LANES) - lax.axis_index("space") * planes
    present = lax.rem(src_ref[0], times) == lax.axis_index("tm")
    present = present & (plane >= 0) & (plane < planes)
    spot = (lax.broadcasted_iota(jnp.int32, (rows, LANES), 0) == lax.div(column, LANES)) & (
        lax.broadcasted_iota(jnp.int32, (rows, LANES), 1) == lax.rem(column, LANES)
    )

    def pick(ref, f):
        value = jnp.zeros((rows, LANES), jnp.float32)
        for p in range(planes):
            here = spot & (plane == p)
            value = value + jnp.where(here, ref[f * (planes + 1) + p], 0.0)
        value = jnp.sum(jnp.sum(value, axis=0, keepdims=True), axis=1, keepdims=True)
        return jnp.broadcast_to(value, (8, LANES))

    anchor = matmul3(
        exponential([pick(slab_two, f) for f in range(FIELDS)]),
        exponential([pick(slab_one, f) for f in range(FIELDS)]),
    )
    pairs = prop_ref.shape[0] // 2
    first_lane = lane_of((1, LANES)) == 0
    for r in range(2):
        for a in range(3):
            for b in range(3):
                e = 2 * pairs + at(r, a, b)
                sum_ref[e : e + 1, :] = jnp.where(
                    first_lane & present, anchor[a][b][r][0:1, :], 0.0
                )
    late[3].wait()
    pause(1e9) if times == 1 else None
    for p in range(planes):
        steps[1].until(1e9, keep=planes - 1 - p)

        @pl.loop(0, rows // 8)
        def _(j):
            band = pl.ds(pl.multiple_of(j * 8, 8), 8)
            two = exponential(
                [
                    relays[1].value((f // plan.ratio) * planes + p, f % plan.ratio, band)
                    for f in range(FIELDS)
                ]
            )
            one = [
                [tuple(ahead_ref[at(r, a, b), p, band, :] for r in range(2)) for b in range(3)]
                for a in range(3)
            ]
            t = matmul3(two, one)
            for q in range(pairs // 3):
                s = [
                    tuple(
                        prop_ref[r * pairs + q * 3 + k, pl.ds(j * 8 * planes + p, 8, planes), :]
                        for r in range(2)
                    )
                    for k in range(3)
                ]
                for a in range(3):
                    re = im = None
                    for k in range(3):
                        x = cmul(t[a][k], s[k])
                        re, im = x if re is None else (re + x[0], im + x[1])
                    acc_ref[q * 3 + a] += re
                    acc_ref[pairs + q * 3 + a] += im

    for e in range(2 * pairs):
        sum_ref[e : e + 1, :] = jnp.sum(acc_ref[e], axis=0, keepdims=True)
    row_ref[...] = lax.dot_general(
        jnp.ones((8, LANES), jnp.float32),
        sum_ref[...],
        (((1,), (1,)), ((), ())),
        precision=EXACT,
        preferred_element_type=jnp.float32,
    )[0:1, :]
    stages[0].run(row_ref)
    if len(stages) == 1:
        for t in range(times):
            value = stages[0].target[t]
            for s in range(1, space):
                value = value + stages[0].target[s * times + t]
            table_ref[t : t + 1, :] = value
    else:
        value = stages[0].target[0]
        for s in range(1, space):
            value = value + stages[0].target[s]
        row_ref[...] = value
        stages[1].run(row_ref)
        for t in range(times):
            table_ref[t : t + 1, :] = stages[1].target[t]
    for swap in swaps:
        swap.drain()
    for relay in relays:
        relay.drain()


def close_kernel(pairs, scale, table_ref, wall_ref, flat_ref):
    times = table_ref.shape[0]
    flat_ref[...] = jnp.zeros_like(flat_ref)
    for t in range(times):
        for r in range(2):
            flat_ref[r : r + 1, t * pairs : (t + 1) * pairs] = table_ref[
                t : t + 1, r * pairs : (r + 1) * pairs
            ]
    length = flat_ref.shape[1]
    entry = jnp.sum(table_ref[...], axis=0, keepdims=True)
    lanes = lax.broadcasted_iota(jnp.int32, (1, length), 1)
    colour = lax.rem(lax.div(lanes, SC), 3)
    re, im = flat_ref[0:1, :], flat_ref[1:2, :]
    real = imag = jnp.zeros((1, length), jnp.float32)
    for gap in range(-2, 3):
        xr = pltpu.roll(re, (gap * SC) % length, 1) if gap else re
        xi = pltpu.roll(im, (gap * SC) % length, 1) if gap else im
        for b in range(3):
            c = b - gap
            if 0 <= c < 3:
                ar, ai = (
                    jnp.broadcast_to(
                        entry[:, 2 * pairs + at(r, b, c) : 2 * pairs + at(r, b, c) + 1],
                        (1, length),
                    )
                    for r in range(2)
                )
                real = real + jnp.where(colour == b, xr * ar + xi * ai, 0.0)
                imag = imag + jnp.where(colour == b, xi * ar - xr * ai, 0.0)
    wall_ref[0:1, :] = real[:, : SC * SC] * scale
    wall_ref[1:2, :] = imag[:, : SC * SC] * scale


def body(sizes, links, propagator, sink_time, src_time, src_site):
    space, times = sizes["space"], sizes["tm"]
    planes, area = links.shape[5], links.shape[6]
    side = math.isqrt(area)
    wide = planes * space
    rows = area // LANES
    assert side * 2 == LANES and rows % 8 == 0

    basis, moment = real_basis(side)
    right, left = plane_matrices(basis)
    back, turn = plane_matrices(basis.T)
    x_basis, x_moment = real_basis(wide)
    yz = (moment.reshape(rows, 2, 1) + moment[None, None, :]).reshape(rows, LANES)
    yz = yz.astype(np.float32)
    plan = Plan(sizes, planes, rows, x_basis, x_moment)

    def fold(x):
        lead = x.shape[:-2]
        x = x.reshape(lead + (planes, rows, LANES))
        return jnp.swapaxes(x, -3, -2).reshape((-1, rows * planes, LANES))

    linked, source = fold(links[0]), fold(propagator)
    pairs = propagator.shape[1]
    assert 2 * pairs + 18 <= LANES
    stages = [("space", "tm")] if space * times <= 64 else [("space",), ("tm",)]
    vmem = lambda *shape: pltpu.VMEM(shape, jnp.float32)
    sems = pltpu.SemaphoreType.DMA
    chunks = plan.groups * planes
    gathers = []
    for axes in stages:
        count = math.prod(sizes[axis] for axis in axes)
        gathers += [vmem(count, 1, LANES), sems((count,)), sems((count,))]
    tables = [right, left, back, turn]
    scratch = [vmem(*linked.shape)]
    scratch += [pltpu.VMEM(m.shape, jnp.bfloat16) for m in tables]
    scratch += [vmem(*yz.shape), vmem(*source.shape), sems((9,))]
    scratch += [vmem(2 * ITERS, *plan.chunk)] * 2
    scratch += [sems((4 * ITERS, plan.groups, space)), vmem(len(plan.levels), 8, LANES)]
    scratch += [vmem(*plan.slab)] * 2 + [vmem(54, planes, rows, LANES)]
    scratch += [vmem(18, planes + 1, rows, LANES), vmem(36, planes, rows, LANES)]
    scratch += [vmem(ITERS, chunks, plan.ratio, rows, LANES)] * 2
    scratch += [sems((ITERS, 4, chunks))]
    scratch += [vmem(2 * pairs, 8, LANES), vmem(LANES, LANES), vmem(1, LANES)]
    final, table = pl.pallas_call(
        functools.partial(main_kernel, plan, stages),
        out_shape=[
            pltpu.VMEM(linked.shape, jnp.float32),
            pltpu.VMEM((times, LANES), jnp.float32),
        ],
        in_specs=[SMEM] * 3 + [ANY] * 7,
        out_specs=[VMEM] * 2,
        scratch_shapes=scratch + gathers,
        compiler_params=pltpu.CompilerParams(
            collective_id=0, has_side_effects=True, vmem_limit_bytes=LIMIT
        ),
    )(sink_time, src_time, src_site, linked, *tables, yz, source)
    wall = pl.pallas_call(
        functools.partial(close_kernel, pairs, float(wide * area) ** (-0.5)),
        out_shape=jax.ShapeDtypeStruct((2, SC * SC), jnp.float32),
        in_specs=[VMEM],
        out_specs=VMEM,
        scratch_shapes=[vmem(8, 2 * LANES)],
    )(pltpu.with_memory_space_constraint(table, pltpu.VMEM))
    final = jnp.swapaxes(final.reshape(54, rows, planes, LANES), 1, 2)
    return final.reshape(links.shape), wall


def solution(mesh):
    sizes = {axis: mesh.shape[axis] for axis in ("space", "tm")}
    placed = (
        P("tm", None, None, None, None, "space", None),
        P(None, "tm", "space", None),
        P(),
        P(),
        P(),
    )
    return jax.shard_map(
        functools.partial(body, sizes),
        mesh=mesh,
        in_specs=placed,
        out_specs=(P("tm", None, None, None, None, "space", None), P()),
        check_vma=False,
    )
```

```python
import functools
import math

import jax
import jax.numpy as jnp
import numpy as np
from jax import lax
from jax.experimental import pallas as pl
from jax.experimental.pallas import tpu as pltpu
from jax.sharding import PartitionSpec as P

SC = 12
ITERS = 2
STEP = 0.08 / 16.0
PEAK = 12.0
LANES = 128
FIELDS = 8
PIECES = 6
EXACT = lax.Precision.HIGHEST
MESH = pl.DeviceIdType.MESH
VMEM = pl.BlockSpec(memory_space=pltpu.VMEM)
HBM = pl.BlockSpec(memory_space=pltpu.HBM)
LIMIT = 60 * 1024 * 1024


def real_basis(n):
    x = np.arange(n)
    rows, moment = [], []
    for k in range(n // 2 + 1):
        angle = 2.0 * np.pi * ((k * x) % n) / n
        square = 4.0 * np.sin(np.pi * k / n) ** 2
        if k == 0 or 2 * k == n:
            rows.append(np.cos(angle) / np.sqrt(n))
            moment.append(square)
        else:
            rows.append(np.cos(angle) * np.sqrt(2.0 / n))
            rows.append(np.sin(angle) * np.sqrt(2.0 / n))
            moment += [square, square]
    return np.array(rows), np.array(moment)


def halves(m):
    high = m.astype(jnp.bfloat16)
    return high, (m - high.astype(np.float64)).astype(jnp.bfloat16)


def plane_matrices(q):
    n = q.shape[0]
    zero = np.zeros((n, n))
    right = np.block([[q.T, zero, zero, q.T], [zero, q.T, q.T, zero]])
    even, odd = q[0::2], q[1::2]
    left = np.block([[even[:, 0::2], even[:, 1::2]], [odd[:, 1::2], odd[:, 0::2]]])
    high, low = halves(right)
    right = np.concatenate([high, high, low], axis=0)
    high, low = halves(left)
    return right, np.concatenate([high, high, low], axis=1)


def triple(x, axis):
    high = x.astype(jnp.bfloat16)
    low = (x - high.astype(jnp.float32)).astype(jnp.bfloat16)
    return jnp.concatenate([high, low, high], axis=axis)


def dot(a, b):
    return jnp.dot(a, b, preferred_element_type=jnp.float32)


def plane_transform(slabs, right, left):
    rows = slabs[0].shape[0]
    wide = dot(triple(jnp.concatenate(slabs, axis=0), 1), right)
    count = len(slabs)
    straight = [wide[i * rows : (i + 1) * rows, :LANES] for i in range(count)]
    swapped = [wide[i * rows : (i + 1) * rows, LANES:] for i in range(count)]
    tall = jnp.concatenate(
        [jnp.concatenate(straight, axis=1), jnp.concatenate(swapped, axis=1)], axis=0
    )
    both = dot(left, triple(tall, 0))
    low = lax.broadcasted_iota(jnp.int32, (rows, LANES), 1) < LANES // 2
    return [
        jnp.where(
            low,
            both[:rows, i * LANES : (i + 1) * LANES],
            both[rows:, i * LANES : (i + 1) * LANES],
        )
        for i in range(count)
    ]


def lane_of(shape):
    return lax.broadcasted_iota(jnp.int32, shape, 1)


def y_behind(v):
    half = LANES // 2
    r = pltpu.roll(v, half, 1)
    return jnp.where(lane_of(v.shape) < half, pltpu.roll(r, 1, 0), r)


def y_ahead(v):
    half = LANES // 2
    r = pltpu.roll(v, half, 1)
    return jnp.where(lane_of(v.shape) < half, r, pltpu.roll(r, v.shape[0] - 1, 0))


def z_behind(v):
    half = LANES // 2
    edge = lane_of(v.shape) % half == 0
    return jnp.where(edge, pltpu.roll(v, half + 1, 1), pltpu.roll(v, 1, 1))


def z_ahead(v):
    half = LANES // 2
    edge = lane_of(v.shape) % half == half - 1
    return jnp.where(edge, pltpu.roll(v, half - 1, 1), pltpu.roll(v, LANES - 1, 1))


PAIRS = ((0, 1), (0, 2), (1, 2))


def project(get, f):
    if f < 6:
        a, b = PAIRS[f % 3]
        if f < 3:
            return 0.5 * (get(0, a, b) - get(0, b, a))
        return 0.5 * (get(1, a, b) + get(1, b, a))
    diag = [get(1, a, a) for a in range(3)]
    return diag[f - 6] - (diag[0] + diag[1] + diag[2]) * (1.0 / 3.0)


def cmul(a, b):
    return (a[0] * b[0] - a[1] * b[1], a[0] * b[1] + a[1] * b[0])


def exponential(fields):
    v = [STEP * f for f in fields]
    h0, h1 = v[6], v[7]
    h2 = -(h0 + h1)
    h01, h02, h12 = (v[3], -v[0]), (v[4], -v[1]), (v[5], -v[2])
    n01 = h01[0] * h01[0] + h01[1] * h01[1]
    n02 = h02[0] * h02[0] + h02[1] * h02[1]
    n12 = h12[0] * h12[0] + h12[1] * h12[1]
    c = 0.5 * (h0 * h0 + h1 * h1 + h2 * h2) + n01 + n02 + n12
    prod = cmul(h01, h12)
    triple = prod[0] * h02[0] + prod[1] * h02[1]
    d = h0 * h1 * h2 + 2.0 * triple - h0 * n12 - h1 * n02 - h2 * n01
    cd, cc, dd = c * d, c * c, d * d
    f0 = (1.0 - dd * (1 / 720), cd * (1 / 120) - d * (1 / 6))
    f1 = (d * (1 / 24) - cd * (1 / 360), 1.0 - c * (1 / 6) + cc * (1 / 120))
    f2 = (c * (1 / 24) - 0.5 - cc * (1 / 720), d * (1 / 120))
    for _ in range(3):
        s00, s01, s02 = cmul(f0, f0), cmul(f0, f1), cmul(f0, f2)
        s11, s12, s22 = cmul(f1, f1), cmul(f1, f2), cmul(f2, f2)
        f0 = tuple(s00[i] + 2.0 * d * s12[i] for i in range(2))
        f1 = tuple(2.0 * (s01[i] + c * s12[i]) + d * s22[i] for i in range(2))
        f2 = tuple(s11[i] + 2.0 * s02[i] + c * s22[i] for i in range(2))
    conj = lambda x: (x[0], -x[1])
    mixed = cmul(h02, conj(h12))
    q01 = (mixed[0] - h2 * h01[0], mixed[1] - h2 * h01[1])
    q02 = (prod[0] - h1 * h02[0], prod[1] - h1 * h02[1])
    mixed = cmul(conj(h01), h02)
    q12 = (mixed[0] - h0 * h12[0], mixed[1] - h0 * h12[1])
    diag = ((h0, h0 * h0 + n01 + n02), (h1, h1 * h1 + n01 + n12), (h2, h2 * h2 + n02 + n12))
    gauge = [[None] * 3 for _ in range(3)]
    for a in range(3):
        h, q = diag[a]
        gauge[a][a] = tuple(f0[i] + f1[i] * h + f2[i] * q for i in range(2))
    for a, b, h, q in ((0, 1, h01, q01), (0, 2, h02, q02), (1, 2, h12, q12)):
        x, y = cmul(f1, h), cmul(f2, q)
        gauge[a][b] = (x[0] + y[0], x[1] + y[1])
        x, y = cmul(f1, conj(h)), cmul(f2, conj(q))
        gauge[b][a] = (x[0] + y[0], x[1] + y[1])
    return gauge


def matmul3(left, right, adjoint=False):
    out = [[None] * 3 for _ in range(3)]
    for a in range(3):
        for b in range(3):
            re = im = None
            for k in range(3):
                xr, xi = left[a][k]
                yr, yi = right[b][k] if adjoint else right[k][b]
                if adjoint:
                    r, i = xr * yr + xi * yi, xi * yr - xr * yi
                else:
                    r, i = xr * yr - xi * yi, xr * yi + xi * yr
                re, im = (r, i) if re is None else (re + r, im + i)
            out[a][b] = (re, im)
    return out


def at(part, a, b):
    return part * 9 + a * 3 + b


class Swap:
    def __init__(self, size, send, recv, send_sem, recv_sem):
        self.size, self.send, self.recv = size, send, recv
        self.send_sem, self.recv_sem = send_sem, recv_sem
        self.me = lax.axis_index("space")

    def copy(self, g, off):
        peer = lax.rem(self.me + off, self.size)
        return pltpu.make_async_remote_copy(
            src_ref=self.send.at[g, peer],
            dst_ref=self.recv.at[g, self.me],
            send_sem=self.send_sem.at[g, off],
            recv_sem=self.recv_sem.at[g, off],
            device_id={"space": peer},
            device_id_type=MESH,
        )

    def start(self, g):
        for off in range(1, self.size):
            self.copy(g, off).start()
        self.recv[g, self.me] = self.send[g, self.me]

    def arrive(self, g):
        for off in range(1, self.size):
            self.copy(g, off).wait_recv()

    def drain(self):
        for g in range(self.send.shape[0]):
            for off in range(1, self.size):
                self.copy(g, off).wait_send()


class Relay:
    def __init__(self, size, root, own, up, down, sems):
        self.size, self.root, self.own = size, root, own
        self.up, self.down = up, down
        self.sems = sems
        self.me = lax.axis_index("tm")
        self.deep = min(size, 4)

    def hop(self, k, rise):
        buffer = self.up if rise else self.down
        base = 0 if rise else 2
        step = 1 if rise else self.size - 1
        return pltpu.make_async_remote_copy(
            src_ref=buffer.at[k],
            dst_ref=buffer.at[k],
            send_sem=self.sems.at[base, k],
            recv_sem=self.sems.at[base + 1, k],
            device_id={"tm": lax.rem(self.me + step, self.size)},
            device_id_type=MESH,
        )

    def step(self, k, h):
        for rise in (True, False):
            place = self.me if rise else self.size - 1 - self.me
            last = h == self.deep - 1
            here = (place >= h) if last else (place == h)
            buffer = self.up if rise else self.down
            parts = buffer.shape[1]

            @pl.when(here)
            def _():
                if h == 0:
                    for j in range(parts):
                        buffer[k, j] = self.own(k, j)
                else:
                    self.hop(k, rise).wait_recv()
                    mine = jnp.broadcast_to(lax.rem(self.root[0], self.size), buffer.shape[2:]) == self.me
                    for j in range(parts):
                        buffer[k, j] = jnp.where(mine, self.own(k, j), buffer[k, j])
                if not last:
                    self.hop(k, rise).start()
                elif self.size > self.deep:

                    @pl.when(place < self.size - 1)
                    def _():
                        self.hop(k, rise).start()

    def drain(self):
        for k in range(self.up.shape[0]):

            @pl.when(self.me < self.size - 1)
            def _():
                self.hop(k, True).wait_send()

            @pl.when(self.me > 0)
            def _():
                self.hop(k, False).wait_send()

    def value(self, k, j, band):
        own = self.own(k, j, band)
        root = jnp.broadcast_to(lax.rem(self.root[0], self.size), own.shape)
        other = jnp.where(root < self.me, self.up[k, j, band, :], self.down[k, j, band, :])
        return jnp.where(root == self.me, own, other)


def greet(sizes):
    barrier = pltpu.get_barrier_semaphore()
    me, time = lax.axis_index("space"), lax.axis_index("tm")
    size, times = sizes["space"], sizes["tm"]

    def signal(peer):
        pl.semaphore_signal(barrier, inc=1, device_id=peer, device_id_type=MESH)

    for off in range(1, size):
        signal({"space": lax.rem(me + off, size)})
    above, below = time < times - 1, time > 0

    @pl.when(above)
    def _():
        signal({"tm": lax.rem(time + 1, times)})

    @pl.when(below)
    def _():
        signal({"tm": lax.rem(time + times - 1, times)})

    return size - 1 + above.astype(jnp.int32) + below.astype(jnp.int32)


class Plan:
    def __init__(self, sizes, planes, rows, basis, moment):
        self.sizes, self.planes, self.rows = sizes, planes, rows
        self.basis, self.moment = basis, moment
        self.size = sizes["space"]
        self.ratio = 8 * self.size // rows
        self.groups = FIELDS // self.ratio
        assert self.ratio * rows == 8 * self.size and self.groups * self.ratio == FIELDS
        self.levels = sorted(set(np.round(moment, 9)))
        self.chunk = (self.groups, self.size, planes + 1, 8, LANES)
        self.slab = (FIELDS * (planes + 1), rows, LANES)

    def fields(self, g):
        return range(g * self.ratio, (g + 1) * self.ratio)


def weigh(plan, yz_ref, weight_ref):
    block = lax.div(lax.axis_index("space"), plan.ratio)
    yz = yz_ref[pl.ds(pl.multiple_of(block * 8, 8), 8), :]
    for index, level in enumerate(plan.levels):
        p2 = yz + float(level)
        if level == 0.0:
            weight = jnp.where(p2 > 0.0, PEAK / jnp.where(p2 > 0.0, p2, 1.0), 0.0)
        else:
            weight = PEAK / p2
        weight_ref[index] = weight


def forward(plan, u, g, right, left, send_ref):
    planes = plan.planes
    slabs = []
    for f in plan.fields(g):
        before = None
        for p in range(planes):
            x, y, z = (
                project(lambda part, a, b, i=i: u(i, part, a, b, p), f) for i in range(3)
            )
            value = (y_behind(y) - y + z_behind(z) - z) - x
            slabs.append(value if before is None else value + before)
            before = x
        slabs.append(before)
    done = plane_transform(slabs, right, left)
    for index, slab in enumerate(done):
        i, p = divmod(index, planes + 1)
        for block in range(plan.rows // 8):
            send_ref[g, block * plan.ratio + i, p] = slab[block * 8 : block * 8 + 8, :]


def backward(plan, g, right, left, recv_ref, slab_ref):
    slabs = []
    for i in range(plan.ratio):
        for p in range(plan.planes + 1):
            slabs.append(
                jnp.concatenate(
                    [recv_ref[g, b * plan.ratio + i, p] for b in range(plan.rows // 8)],
                    axis=0,
                )
            )
    base = g * plan.ratio * (plan.planes + 1)
    for index, slab in enumerate(plane_transform(slabs, right, left)):
        slab_ref[base + index] = slab


def across(plan, g, recv_ref, weight_ref, send_ref):
    planes, count, basis = plan.planes, plan.size, plan.basis
    n = basis.shape[0]
    v = []
    for s in range(count):
        for p in range(planes):
            value = recv_ref[g, s, p]
            if p == 0:
                value = value + recv_ref[g, (s - 1) % count, planes]
            v.append(value)
    half = range(1, (n + 1) // 2)
    even = {0: v[0]}
    odd = {}
    if n % 2 == 0:
        even[n // 2] = v[n // 2]
    for x in half:
        even[x] = v[x] + v[n - x]
        odd[x] = v[x] - v[n - x]
    back_even = {x: None for x in even}
    back_odd = {x: None for x in odd}
    for k in range(n):
        is_sine = abs(basis[k, 0]) < 1e-9
        source, target = (odd, back_odd) if is_sine else (even, back_even)
        mode = None
        for x in source:
            term = float(basis[k, x]) * source[x]
            mode = term if mode is None else mode + term
        mode = mode * weight_ref[plan.levels.index(np.round(plan.moment[k], 9))]
        for x in target:
            term = float(basis[k, x]) * mode
            target[x] = term if target[x] is None else target[x] + term
    out = [None] * n
    for x in back_even:
        out[x] = back_even[x]
    for x in half:
        out[x] = back_even[x] + back_odd[x]
        out[n - x] = back_even[x] - back_odd[x]
    for d in range(count):
        for p in range(planes + 1):
            send_ref[g, d, p] = out[(d * planes + p) % n]


def gauge_of(slab_ref, planes, gauge_ref):
    rows = gauge_ref.shape[2]

    for p in range(planes + 1):

        @pl.loop(0, rows // 8)
        def _(j):
            band = pl.ds(pl.multiple_of(j * 8, 8), 8)
            g = exponential([slab_ref[f * (planes + 1) + p, band, :] for f in range(FIELDS)])
            for a in range(3):
                for b in range(3):
                    for part in range(2):
                        gauge_ref[at(part, a, b), p, band, :] = g[a][b][part]


def shift_all(planes, gauge_ref, ahead_ref):
    for e in range(18):
        for p in range(planes):
            ahead_ref[e, p] = y_ahead(gauge_ref[e, p])
            ahead_ref[18 + e, p] = z_ahead(gauge_ref[e, p])


def rotate_plane(get_band, put_band, p, gauge_ref, ahead_ref):
    rows = gauge_ref.shape[2]

    @pl.loop(0, rows // 8)
    def _(j):
        start = pl.multiple_of(j * 8, 8)
        band = pl.ds(start, 8)
        for i in range(3):
            g = [
                [tuple(gauge_ref[at(r, a, b), p, band, :] for r in range(2)) for b in range(3)]
                for a in range(3)
            ]
            u = [
                [tuple(get_band(i, r, a, b, p, j) for r in range(2)) for b in range(3)]
                for a in range(3)
            ]
            if i == 0:
                source = lambda r, a, b: gauge_ref[at(r, a, b), p + 1, band, :]
            else:
                source = lambda r, a, b: ahead_ref[(i - 1) * 18 + at(r, a, b), p, band, :]
            ahead = [
                [tuple(source(r, a, b) for r in range(2)) for b in range(3)]
                for a in range(3)
            ]
            out = matmul3(matmul3(g, u), ahead, adjoint=True)
            for a in range(3):
                for b in range(3):
                    for r in range(2):
                        put_band(i, r, a, b, p, j, out[a][b][r])


class Steps:
    def __init__(self, relay, start):
        self.relay, self.start = relay, start
        chunks = relay.up.shape[0]
        self.left = sorted(
            [(k, h) for k in range(chunks) for h in range(1, relay.deep)], key=self.ready
        )

    def ready(self, step):
        return self.start + 0.7 * step[0] + 2.8 * step[1]

    def until(self, time, keep=0):
        while len(self.left) > keep and self.ready(self.left[0]) <= time:
            self.relay.step(*self.left.pop(0))


class Gather:
    def __init__(self, sizes, axes, target, send, recv):
        self.axes, self.target, self.send, self.recv = axes, target, send, recv
        me = [lax.axis_index(axis) for axis in axes]
        extent = [sizes[axis] for axis in axes]
        slot = 0
        for index, size in zip(me, extent):
            slot = slot * size + index
        self.slot = slot
        self.peers = []
        for flat in range(1, math.prod(extent)):
            rest, peer = flat, {}
            for axis, index, size in reversed(list(zip(axes, me, extent))):
                peer[axis] = lax.rem(index + rest % size, size)
                rest //= size
            self.peers.append((flat, peer))

    def run(self, source):
        copies = []
        for flat, peer in self.peers:
            copies.append(
                pltpu.make_async_remote_copy(
                    src_ref=source,
                    dst_ref=self.target.at[self.slot],
                    send_sem=self.send.at[flat],
                    recv_sem=self.recv.at[flat],
                    device_id=peer,
                    device_id_type=MESH,
                )
            )
            copies[-1].start()
        self.target[self.slot] = source[...]
        for copy in copies:
            copy.wait()


def main_kernel(
    plan, stages, sink_any, src_any, site_any, links_any, right_any, left_any, back_any,
    turn_any, yz_any, prop_any,
    out_ref, table_ref,
    sink_ref, src_ref, site_ref,
    links_ref, right_ref, left_ref, back_ref, turn_ref, yz_ref, prop_ref, load_sems,
    send_ref, recv_ref, swap_sems, weight_ref, slab_one, slab_two, lattice_ref,
    gauge_ref, ahead_ref, up_ref, down_ref, relay_sems, acc_ref, sum_ref, row_ref, *gathers,
):
    planes, rows, sizes = plan.planes, plan.rows, plan.sizes
    space, times = sizes["space"], sizes["tm"]
    stages = [
        Gather(sizes, axes, *gathers[3 * i : 3 * i + 3]) for i, axes in enumerate(stages)
    ]
    total = greet(sizes)

    pairs_of = [
        (right_any, right_ref), (left_any, left_ref), (back_any, back_ref),
        (turn_any, turn_ref), (yz_any, yz_ref), (sink_any, sink_ref), (src_any, src_ref),
        (site_any, site_ref), (prop_any, prop_ref),
    ]
    early = [
        pltpu.make_async_copy(
            links_any.at[pl.ds(i * 18, 18)], links_ref.at[pl.ds(i * 18, 18)], load_sems.at[i]
        )
        for i in range(3)
    ]
    late = [
        pltpu.make_async_copy(a, b, load_sems.at[3 + i]) for i, (a, b) in enumerate(pairs_of)
    ]
    early += late[:2]
    late = late[2:]
    for copy in early + late:
        copy.start()

    swaps = [
        Swap(space, send_ref.at[i], recv_ref.at[i], swap_sems.at[2 * i], swap_sems.at[2 * i + 1])
        for i in range(2 * ITERS)
    ]

    def owner(slab):
        def own(k, j, band=slice(None)):
            g, p = divmod(k, planes)
            return slab[(g * plan.ratio + j) * (planes + 1) + p, band, :]

        return own

    relays = [
        Relay(times, sink_ref, owner(slab), up_ref.at[i], down_ref.at[i], relay_sems.at[i])
        for i, slab in enumerate((slab_one, slab_two))
    ]
    steps = [Steps(relay, 0.8) for relay in relays]

    def sweep(u, index, before=lambda: None):
        one, two = swaps[2 * index], swaps[2 * index + 1]
        slab, relay = (slab_one, slab_two)[index], relays[index]
        for g in range(plan.groups):
            forward(plan, u, g, right_ref[...], left_ref[...], one.send)
            if g == 0:
                before()
            one.start(g)
            if index:
                steps[0].until(6.5 + 0.3 * g)
        if index == 0:
            for copy in late[:-1]:
                copy.wait()
            weigh(plan, yz_ref, weight_ref)
        for g in range(plan.groups):
            if index:
                steps[0].until(10.6 + 1.05 * g)
            one.arrive(g)
            across(plan, g, one.recv, weight_ref, two.send)
            two.start(g)
        if index:
            steps[0].until(1e9)
        for g in range(plan.groups):
            two.arrive(g)
            backward(plan, g, back_ref[...], turn_ref[...], two.recv, slab)
            for p in range(planes):
                relay.step(g * planes + p, 0)

    for copy in early:
        copy.wait()

    def first(i, part, a, b, p):
        return links_ref[i * 18 + at(part, a, b), pl.ds(p, rows, planes), :]

    sweep(first, 0, lambda: pl.semaphore_wait(pltpu.get_barrier_semaphore(), total))
    steps[0].until(3.6)
    gauge_of(slab_one, planes, gauge_ref)
    steps[0].until(4.3)
    shift_all(planes, gauge_ref, ahead_ref)

    def get(i, r, a, b, p, j):
        return links_ref[i * 18 + at(r, a, b), pl.ds(j * 8 * planes + p, 8, planes), :]

    def put(i, r, a, b, p, j, value):
        lattice_ref[i * 18 + at(r, a, b), p, pl.ds(pl.multiple_of(j * 8, 8), 8), :] = value

    for p in range(planes):
        rotate_plane(get, put, p, gauge_ref, ahead_ref)
        steps[0].until(5.3 + 0.7 * p)

    sweep(lambda i, part, a, b, p: lattice_ref[i * 18 + at(part, a, b), p], 1)

    time = [3.6]

    def pause(length):
        time[0] += length
        steps[1].until(time[0])

    pause(0.0)
    gauge_of(slab_two, planes, gauge_ref)
    pause(0.7)
    shift_all(planes, gauge_ref, ahead_ref)
    pause(0.4)

    def get_last(i, r, a, b, p, j):
        return lattice_ref[i * 18 + at(r, a, b), p, pl.ds(pl.multiple_of(j * 8, 8), 8), :]

    def put_last(i, r, a, b, p, j, value):
        out_ref[i * 18 + at(r, a, b), pl.ds(j * 8 * planes + p, 8, planes), :] = value

    for p in range(planes):
        rotate_plane(get_last, put_last, p, gauge_ref, ahead_ref)
        pause(0.7)
    for p in range(planes):

        @pl.loop(0, rows // 8)
        def _(j):
            band = pl.ds(pl.multiple_of(j * 8, 8), 8)
            one = exponential(
                [
                    relays[0].value((f // plan.ratio) * planes + p, f % plan.ratio, band)
                    for f in range(FIELDS)
                ]
            )
            for a in range(3):
                for b in range(3):
                    for part in range(2):
                        ahead_ref[at(part, a, b), p, band, :] = one[a][b][part]

    pause(0.6)
    for swap in swaps:
        swap.drain()
    acc_ref[...] = jnp.zeros_like(acc_ref)
    sum_ref[...] = jnp.zeros_like(sum_ref)
    site = site_ref[0]
    column = lax.rem(site, rows * LANES)
    plane = lax.div(site, rows * LANES) - lax.axis_index("space") * planes
    present = lax.rem(src_ref[0], times) == lax.axis_index("tm")
    present = present & (plane >= 0) & (plane < planes)
    spot = (lax.broadcasted_iota(jnp.int32, (rows, LANES), 0) == lax.div(column, LANES)) & (
        lax.broadcasted_iota(jnp.int32, (rows, LANES), 1) == lax.rem(column, LANES)
    )

    def pick(ref, f):
        value = jnp.zeros((rows, LANES), jnp.float32)
        for p in range(planes):
            here = spot & (plane == p)
            value = value + jnp.where(here, ref[f * (planes + 1) + p], 0.0)
        value = jnp.sum(jnp.sum(value, axis=0, keepdims=True), axis=1, keepdims=True)
        return jnp.broadcast_to(value, (8, LANES))

    anchor = matmul3(
        exponential([pick(slab_two, f) for f in range(FIELDS)]),
        exponential([pick(slab_one, f) for f in range(FIELDS)]),
    )
    pairs = prop_ref.shape[0] // 2
    first_lane = lane_of((1, LANES)) == 0
    for r in range(2):
        for a in range(3):
            for b in range(3):
                e = 2 * pairs + at(r, a, b)
                sum_ref[e : e + 1, :] = jnp.where(
                    first_lane & present, anchor[a][b][r][0:1, :], 0.0
                )
    late[-1].wait()
    pause(1e9) if times == 1 else None
    for p in range(planes):
        steps[1].until(1e9, keep=planes - 1 - p)

        @pl.loop(0, rows // 8)
        def _(j):
            band = pl.ds(pl.multiple_of(j * 8, 8), 8)
            two = exponential(
                [
                    relays[1].value((f // plan.ratio) * planes + p, f % plan.ratio, band)
                    for f in range(FIELDS)
                ]
            )
            one = [
                [tuple(ahead_ref[at(r, a, b), p, band, :] for r in range(2)) for b in range(3)]
                for a in range(3)
            ]
            t = matmul3(two, one)
            for q in range(pairs // 3):
                s = [
                    tuple(
                        prop_ref[r * pairs + q * 3 + k, pl.ds(j * 8 * planes + p, 8, planes), :]
                        for r in range(2)
                    )
                    for k in range(3)
                ]
                for a in range(3):
                    re = im = None
                    for k in range(3):
                        x = cmul(t[a][k], s[k])
                        re, im = x if re is None else (re + x[0], im + x[1])
                    acc_ref[q * 3 + a] += re
                    acc_ref[pairs + q * 3 + a] += im

    for e in range(2 * pairs):
        sum_ref[e : e + 1, :] = jnp.sum(acc_ref[e], axis=0, keepdims=True)
    row_ref[...] = lax.dot_general(
        jnp.ones((8, LANES), jnp.float32),
        sum_ref[...],
        (((1,), (1,)), ((), ())),
        precision=EXACT,
        preferred_element_type=jnp.float32,
    )[0:1, :]
    stages[0].run(row_ref)
    if len(stages) == 1:
        for t in range(times):
            value = stages[0].target[t]
            for s in range(1, space):
                value = value + stages[0].target[s * times + t]
            table_ref[t : t + 1, :] = value
    else:
        value = stages[0].target[0]
        for s in range(1, space):
            value = value + stages[0].target[s]
        row_ref[...] = value
        stages[1].run(row_ref)
        for t in range(times):
            table_ref[t : t + 1, :] = stages[1].target[t]
    for relay in relays:
        relay.drain()


def close_kernel(pairs, scale, final_ref, table_ref, out_ref, wall_ref, flat_ref, sem):
    share = final_ref.shape[0] // PIECES
    copies = [
        pltpu.make_async_copy(
            final_ref.at[pl.ds(i * share, share)], out_ref.at[pl.ds(i * share, share)], sem.at[i]
        )
        for i in range(PIECES)
    ]
    for copy in copies:
        copy.start()
    times = table_ref.shape[0]
    flat_ref[...] = jnp.zeros_like(flat_ref)
    for t in range(times):
        for r in range(2):
            flat_ref[r : r + 1, t * pairs : (t + 1) * pairs] = table_ref[
                t : t + 1, r * pairs : (r + 1) * pairs
            ]
    length = flat_ref.shape[1]
    entry = jnp.sum(table_ref[...], axis=0, keepdims=True)
    lanes = lax.broadcasted_iota(jnp.int32, (1, length), 1)
    colour = lax.rem(lax.div(lanes, SC), 3)
    re, im = flat_ref[0:1, :], flat_ref[1:2, :]
    real = imag = jnp.zeros((1, length), jnp.float32)
    for gap in range(-2, 3):
        xr = pltpu.roll(re, (gap * SC) % length, 1) if gap else re
        xi = pltpu.roll(im, (gap * SC) % length, 1) if gap else im
        for b in range(3):
            c = b - gap
            if 0 <= c < 3:
                ar, ai = (
                    jnp.broadcast_to(
                        entry[:, 2 * pairs + at(r, b, c) : 2 * pairs + at(r, b, c) + 1],
                        (1, length),
                    )
                    for r in range(2)
                )
                real = real + jnp.where(colour == b, xr * ar + xi * ai, 0.0)
                imag = imag + jnp.where(colour == b, xi * ar - xr * ai, 0.0)
    wall_ref[0:1, :] = real[:, : SC * SC] * scale
    wall_ref[1:2, :] = imag[:, : SC * SC] * scale
    for copy in copies:
        copy.wait()


def body(sizes, links, propagator, sink_time, src_time, src_site):
    space, times = sizes["space"], sizes["tm"]
    planes, area = links.shape[5], links.shape[6]
    side = math.isqrt(area)
    wide = planes * space
    rows = area // LANES
    assert side * 2 == LANES and rows % 8 == 0

    basis, moment = real_basis(side)
    right, left = plane_matrices(basis)
    back, turn = plane_matrices(basis.T)
    x_basis, x_moment = real_basis(wide)
    yz = (moment.reshape(rows, 2, 1) + moment[None, None, :]).reshape(rows, LANES)
    yz = yz.astype(np.float32)
    plan = Plan(sizes, planes, rows, x_basis, x_moment)

    def fold(x):
        lead = x.shape[:-2]
        x = x.reshape(lead + (planes, rows, LANES))
        return jnp.swapaxes(x, -3, -2).reshape((-1, rows * planes, LANES))

    linked, source = fold(links[0]), fold(propagator)
    pairs = propagator.shape[1]
    assert 2 * pairs + 18 <= LANES
    stages = [("space", "tm")] if space * times <= 64 else [("space",), ("tm",)]
    vmem = lambda *shape: pltpu.VMEM(shape, jnp.float32)
    sems = pltpu.SemaphoreType.DMA
    chunks = plan.groups * planes
    gathers = []
    for axes in stages:
        count = math.prod(sizes[axis] for axis in axes)
        gathers += [vmem(count, 1, LANES), sems((count,)), sems((count,))]
    tables = [right, left, back, turn]
    scratch = [pltpu.SMEM((1,), jnp.int32)] * 3 + [vmem(*linked.shape)]
    scratch += [pltpu.VMEM(m.shape, jnp.bfloat16) for m in tables]
    scratch += [vmem(*yz.shape), vmem(*source.shape), sems((12,))]
    scratch += [vmem(2 * ITERS, *plan.chunk)] * 2
    scratch += [sems((4 * ITERS, plan.groups, space)), vmem(len(plan.levels), 8, LANES)]
    scratch += [vmem(*plan.slab)] * 2 + [vmem(54, planes, rows, LANES)]
    scratch += [vmem(18, planes + 1, rows, LANES), vmem(36, planes, rows, LANES)]
    scratch += [vmem(ITERS, chunks, plan.ratio, rows, LANES)] * 2
    scratch += [sems((ITERS, 4, chunks))]
    scratch += [vmem(2 * pairs, 8, LANES), vmem(LANES, LANES), vmem(1, LANES)]
    final, table = pl.pallas_call(
        functools.partial(main_kernel, plan, stages),
        out_shape=[
            pltpu.VMEM(linked.shape, jnp.float32),
            pltpu.VMEM((times, LANES), jnp.float32),
        ],
        in_specs=[HBM] * 10,
        out_specs=[VMEM] * 2,
        scratch_shapes=scratch + gathers,
        compiler_params=pltpu.CompilerParams(
            collective_id=0, has_side_effects=True, vmem_limit_bytes=LIMIT
        ),
    )(sink_time, src_time, src_site, linked, *tables, yz, source)
    final, wall = pl.pallas_call(
        functools.partial(close_kernel, pairs, float(wide * area) ** (-0.5)),
        out_shape=[
            jax.ShapeDtypeStruct(linked.shape, jnp.float32),
            jax.ShapeDtypeStruct((2, SC * SC), jnp.float32),
        ],
        in_specs=[VMEM] * 2,
        out_specs=[HBM, VMEM],
        scratch_shapes=[vmem(8, 2 * LANES), sems((PIECES,))],
    )(*(pltpu.with_memory_space_constraint(x, pltpu.VMEM) for x in (final, table)))
    final = jnp.swapaxes(final.reshape(54, rows, planes, LANES), 1, 2)
    return final.reshape(links.shape), wall


def solution(mesh):
    sizes = {axis: mesh.shape[axis] for axis in ("space", "tm")}
    placed = (
        P("tm", None, None, None, None, "space", None),
        P(None, "tm", "space", None),
        P(),
        P(),
        P(),
    )
    return jax.shard_map(
        functools.partial(body, sizes),
        mesh=mesh,
        in_specs=placed,
        out_specs=(P("tm", None, None, None, None, "space", None), P()),
        check_vma=False,
    )
```

```python
import functools
import math

import jax
import jax.numpy as jnp
import numpy as np
from jax import lax
from jax.experimental import pallas as pl
from jax.experimental.pallas import tpu as pltpu
from jax.sharding import PartitionSpec as P

SC = 12
ITERS = 2
STEP = 0.08 / 16.0
PEAK = 12.0
LANES = 128
FIELDS = 8
PIECES = 6
EXACT = lax.Precision.HIGHEST
MESH = pl.DeviceIdType.MESH
VMEM = pl.BlockSpec(memory_space=pltpu.VMEM)
HBM = pl.BlockSpec(memory_space=pltpu.HBM)
LIMIT = 60 * 1024 * 1024


def real_basis(n):
    x = np.arange(n)
    rows, moment = [], []
    for k in range(n // 2 + 1):
        angle = 2.0 * np.pi * ((k * x) % n) / n
        square = 4.0 * np.sin(np.pi * k / n) ** 2
        if k == 0 or 2 * k == n:
            rows.append(np.cos(angle) / np.sqrt(n))
            moment.append(square)
        else:
            rows.append(np.cos(angle) * np.sqrt(2.0 / n))
            rows.append(np.sin(angle) * np.sqrt(2.0 / n))
            moment += [square, square]
    return np.array(rows), np.array(moment)


def halves(m):
    high = m.astype(jnp.bfloat16)
    return high, (m - high.astype(np.float64)).astype(jnp.bfloat16)


def plane_matrices(q):
    n = q.shape[0]
    zero = np.zeros((n, n))
    right = np.block([[q.T, zero, zero, q.T], [zero, q.T, q.T, zero]])
    even, odd = q[0::2], q[1::2]
    left = np.block([[even[:, 0::2], even[:, 1::2]], [odd[:, 1::2], odd[:, 0::2]]])
    high, low = halves(right)
    right = np.concatenate([high, high, low], axis=0)
    high, low = halves(left)
    return right, np.concatenate([high, high, low], axis=1)


def triple(x, axis):
    high = x.astype(jnp.bfloat16)
    low = (x - high.astype(jnp.float32)).astype(jnp.bfloat16)
    return jnp.concatenate([high, low, high], axis=axis)


def dot(a, b):
    return jnp.dot(a, b, preferred_element_type=jnp.float32)


def plane_transform(slabs, right, left):
    rows = slabs[0].shape[0]
    wide = dot(triple(jnp.concatenate(slabs, axis=0), 1), right)
    count = len(slabs)
    straight = [wide[i * rows : (i + 1) * rows, :LANES] for i in range(count)]
    swapped = [wide[i * rows : (i + 1) * rows, LANES:] for i in range(count)]
    tall = jnp.concatenate(
        [jnp.concatenate(straight, axis=1), jnp.concatenate(swapped, axis=1)], axis=0
    )
    both = dot(left, triple(tall, 0))
    low = lax.broadcasted_iota(jnp.int32, (rows, LANES), 1) < LANES // 2
    return [
        jnp.where(
            low,
            both[:rows, i * LANES : (i + 1) * LANES],
            both[rows:, i * LANES : (i + 1) * LANES],
        )
        for i in range(count)
    ]


def lane_of(shape):
    return lax.broadcasted_iota(jnp.int32, shape, 1)


def y_behind(v):
    half = LANES // 2
    r = pltpu.roll(v, half, 1)
    return jnp.where(lane_of(v.shape) < half, pltpu.roll(r, 1, 0), r)


def y_ahead(v):
    half = LANES // 2
    r = pltpu.roll(v, half, 1)
    return jnp.where(lane_of(v.shape) < half, r, pltpu.roll(r, v.shape[0] - 1, 0))


def z_behind(v):
    half = LANES // 2
    edge = lane_of(v.shape) % half == 0
    return jnp.where(edge, pltpu.roll(v, half + 1, 1), pltpu.roll(v, 1, 1))


def z_ahead(v):
    half = LANES // 2
    edge = lane_of(v.shape) % half == half - 1
    return jnp.where(edge, pltpu.roll(v, half - 1, 1), pltpu.roll(v, LANES - 1, 1))


PAIRS = ((0, 1), (0, 2), (1, 2))


def project(get, f):
    if f < 6:
        a, b = PAIRS[f % 3]
        if f < 3:
            return 0.5 * (get(0, a, b) - get(0, b, a))
        return 0.5 * (get(1, a, b) + get(1, b, a))
    diag = [get(1, a, a) for a in range(3)]
    return diag[f - 6] - (diag[0] + diag[1] + diag[2]) * (1.0 / 3.0)


def cmul(a, b):
    return (a[0] * b[0] - a[1] * b[1], a[0] * b[1] + a[1] * b[0])


def exponential(fields):
    v = [STEP * f for f in fields]
    h0, h1 = v[6], v[7]
    h2 = -(h0 + h1)
    h01, h02, h12 = (v[3], -v[0]), (v[4], -v[1]), (v[5], -v[2])
    n01 = h01[0] * h01[0] + h01[1] * h01[1]
    n02 = h02[0] * h02[0] + h02[1] * h02[1]
    n12 = h12[0] * h12[0] + h12[1] * h12[1]
    c = 0.5 * (h0 * h0 + h1 * h1 + h2 * h2) + n01 + n02 + n12
    prod = cmul(h01, h12)
    triple = prod[0] * h02[0] + prod[1] * h02[1]
    d = h0 * h1 * h2 + 2.0 * triple - h0 * n12 - h1 * n02 - h2 * n01
    cd, cc, dd = c * d, c * c, d * d
    f0 = (1.0 - dd * (1 / 720), cd * (1 / 120) - d * (1 / 6))
    f1 = (d * (1 / 24) - cd * (1 / 360), 1.0 - c * (1 / 6) + cc * (1 / 120))
    f2 = (c * (1 / 24) - 0.5 - cc * (1 / 720), d * (1 / 120))
    for _ in range(3):
        s00, s01, s02 = cmul(f0, f0), cmul(f0, f1), cmul(f0, f2)
        s11, s12, s22 = cmul(f1, f1), cmul(f1, f2), cmul(f2, f2)
        f0 = tuple(s00[i] + 2.0 * d * s12[i] for i in range(2))
        f1 = tuple(2.0 * (s01[i] + c * s12[i]) + d * s22[i] for i in range(2))
        f2 = tuple(s11[i] + 2.0 * s02[i] + c * s22[i] for i in range(2))
    conj = lambda x: (x[0], -x[1])
    mixed = cmul(h02, conj(h12))
    q01 = (mixed[0] - h2 * h01[0], mixed[1] - h2 * h01[1])
    q02 = (prod[0] - h1 * h02[0], prod[1] - h1 * h02[1])
    mixed = cmul(conj(h01), h02)
    q12 = (mixed[0] - h0 * h12[0], mixed[1] - h0 * h12[1])
    diag = ((h0, h0 * h0 + n01 + n02), (h1, h1 * h1 + n01 + n12), (h2, h2 * h2 + n02 + n12))
    gauge = [[None] * 3 for _ in range(3)]
    for a in range(3):
        h, q = diag[a]
        gauge[a][a] = tuple(f0[i] + f1[i] * h + f2[i] * q for i in range(2))
    for a, b, h, q in ((0, 1, h01, q01), (0, 2, h02, q02), (1, 2, h12, q12)):
        x, y = cmul(f1, h), cmul(f2, q)
        gauge[a][b] = (x[0] + y[0], x[1] + y[1])
        x, y = cmul(f1, conj(h)), cmul(f2, conj(q))
        gauge[b][a] = (x[0] + y[0], x[1] + y[1])
    return gauge


def matmul3(left, right, adjoint=False):
    out = [[None] * 3 for _ in range(3)]
    for a in range(3):
        for b in range(3):
            re = im = None
            for k in range(3):
                xr, xi = left[a][k]
                yr, yi = right[b][k] if adjoint else right[k][b]
                if adjoint:
                    r, i = xr * yr + xi * yi, xi * yr - xr * yi
                else:
                    r, i = xr * yr - xi * yi, xr * yi + xi * yr
                re, im = (r, i) if re is None else (re + r, im + i)
            out[a][b] = (re, im)
    return out


def at(part, a, b):
    return part * 9 + a * 3 + b


class Swap:
    def __init__(self, size, send, recv, send_sem, recv_sem):
        self.size, self.send, self.recv = size, send, recv
        self.send_sem, self.recv_sem = send_sem, recv_sem
        self.me = lax.axis_index("space")

    def copy(self, g, off):
        peer = lax.rem(self.me + off, self.size)
        return pltpu.make_async_remote_copy(
            src_ref=self.send.at[g, peer],
            dst_ref=self.recv.at[g, self.me],
            send_sem=self.send_sem.at[g, off],
            recv_sem=self.recv_sem.at[g, off],
            device_id={"space": peer},
            device_id_type=MESH,
        )

    def start(self, g):
        for off in range(1, self.size):
            self.copy(g, off).start()
        self.recv[g, self.me] = self.send[g, self.me]

    def arrive(self, g):
        for off in range(1, self.size):
            self.copy(g, off).wait_recv()

    def drain(self):
        for g in range(self.send.shape[0]):
            for off in range(1, self.size):
                self.copy(g, off).wait_send()


class Relay:
    def __init__(self, size, root, own, up, down, sems):
        self.size, self.root, self.own = size, root, own
        self.up, self.down = up, down
        self.sems = sems
        self.me = lax.axis_index("tm")
        self.deep = min(size, 4)

    def hop(self, k, rise):
        buffer = self.up if rise else self.down
        base = 0 if rise else 2
        step = 1 if rise else self.size - 1
        return pltpu.make_async_remote_copy(
            src_ref=buffer.at[k],
            dst_ref=buffer.at[k],
            send_sem=self.sems.at[base, k],
            recv_sem=self.sems.at[base + 1, k],
            device_id={"tm": lax.rem(self.me + step, self.size)},
            device_id_type=MESH,
        )

    def step(self, k, h):
        for rise in (True, False):
            place = self.me if rise else self.size - 1 - self.me
            last = h == self.deep - 1
            here = (place >= h) if last else (place == h)
            buffer = self.up if rise else self.down
            parts = buffer.shape[1]

            @pl.when(here)
            def _():
                if h == 0:
                    for j in range(parts):
                        buffer[k, j] = self.own(k, j)
                else:
                    self.hop(k, rise).wait_recv()
                    mine = jnp.broadcast_to(lax.rem(self.root[0], self.size), buffer.shape[2:]) == self.me
                    for j in range(parts):
                        buffer[k, j] = jnp.where(mine, self.own(k, j), buffer[k, j])
                if not last:
                    self.hop(k, rise).start()
                elif self.size > self.deep:

                    @pl.when(place < self.size - 1)
                    def _():
                        self.hop(k, rise).start()

    def drain(self):
        for k in range(self.up.shape[0]):

            @pl.when(self.me < self.size - 1)
            def _():
                self.hop(k, True).wait_send()

            @pl.when(self.me > 0)
            def _():
                self.hop(k, False).wait_send()

    def value(self, k, j, band):
        own = self.own(k, j, band)
        root = jnp.broadcast_to(lax.rem(self.root[0], self.size), own.shape)
        other = jnp.where(root < self.me, self.up[k, j, band, :], self.down[k, j, band, :])
        return jnp.where(root == self.me, own, other)


def greet(sizes):
    barrier = pltpu.get_barrier_semaphore()
    me, time = lax.axis_index("space"), lax.axis_index("tm")
    size, times = sizes["space"], sizes["tm"]

    def signal(peer):
        pl.semaphore_signal(barrier, inc=1, device_id=peer, device_id_type=MESH)

    for off in range(1, size):
        signal({"space": lax.rem(me + off, size)})
    above, below = time < times - 1, time > 0

    @pl.when(above)
    def _():
        signal({"tm": lax.rem(time + 1, times)})

    @pl.when(below)
    def _():
        signal({"tm": lax.rem(time + times - 1, times)})

    return size - 1 + above.astype(jnp.int32) + below.astype(jnp.int32)


class Plan:
    def __init__(self, sizes, planes, rows, basis, moment):
        self.sizes, self.planes, self.rows = sizes, planes, rows
        self.basis, self.moment = basis, moment
        self.size = sizes["space"]
        self.ratio = 8 * self.size // rows
        self.groups = FIELDS // self.ratio
        assert self.ratio * rows == 8 * self.size and self.groups * self.ratio == FIELDS
        self.levels = sorted(set(np.round(moment, 9)))
        assert planes == 2
        self.chunk = (self.groups, self.size, planes, 8, LANES)
        self.slab = (FIELDS * (planes + 1), rows, LANES)

    def fields(self, g):
        return range(g * self.ratio, (g + 1) * self.ratio)


def weigh(plan, yz_ref, weight_ref):
    block = lax.div(lax.axis_index("space"), plan.ratio)
    yz = yz_ref[pl.ds(pl.multiple_of(block * 8, 8), 8), :]
    above = PEAK * (yz + 2.0)
    base = yz * (yz + 4.0)
    for index, level in enumerate(plan.levels):
        p2 = base + float(level)
        if level == 0.0:
            weight = jnp.where(p2 > 0.0, above / jnp.where(p2 > 0.0, p2, 1.0), 0.0)
        else:
            weight = above / p2
        weight_ref[index] = weight


def origin(shape, block=0):
    row = lax.broadcasted_iota(jnp.int32, shape, 0) + block
    return (row == 0) & (lane_of(shape) == 0)


def forward(plan, u, g, right, left, ratio_ref, odd_ref, send_ref):
    planes = plan.planes
    slabs = []
    for f in plan.fields(g):
        before = None
        for p in range(planes):
            x, y, z = (
                project(lambda part, a, b, i=i: u(i, part, a, b, p), f) for i in range(3)
            )
            value = (y_behind(y) - y + z_behind(z) - z) - x
            slabs.append(value if before is None else value + before)
            before = x
        slabs.append(before)
    done = plane_transform(slabs, right, left)
    ratio = ratio_ref[...]
    for i, f in enumerate(plan.fields(g)):
        even, odd, edge = done[3 * i : 3 * i + 3]
        odd_ref[f] = odd
        share = ratio * odd
        own, other = even + share, jnp.where(origin(odd.shape), odd, edge + share)
        for block in range(plan.rows // 8):
            band = slice(block * 8, block * 8 + 8)
            send_ref[g, block * plan.ratio + i, 0] = own[band, :]
            send_ref[g, block * plan.ratio + i, 1] = other[band, :]


def backward(plan, g, right, left, ratio_ref, odd_ref, recv_ref, slab_ref):
    slabs = []
    ratio = ratio_ref[...]
    for i, f in enumerate(plan.fields(g)):
        here, ahead = (
            jnp.concatenate(
                [recv_ref[g, b * plan.ratio + i, p] for b in range(plan.rows // 8)], axis=0
            )
            for p in range(2)
        )
        slabs += [here, (PEAK * odd_ref[f] + here + ahead) * ratio, ahead]
    base = g * plan.ratio * (plan.planes + 1)
    for index, slab in enumerate(plane_transform(slabs, right, left)):
        slab_ref[base + index] = slab


def across(plan, g, recv_ref, weight_ref, send_ref):
    n, basis = plan.size, plan.basis
    zero = origin((8, LANES), lax.div(lax.axis_index("space"), plan.ratio))
    own = [recv_ref[g, s, 0] for s in range(n)]
    other = [recv_ref[g, s, 1] for s in range(n)]
    shift = other[0]
    for s in range(1, n):
        shift = shift + other[s]
    shift = jnp.where(zero, shift * (-0.25 * PEAK / n), 0.0)
    other = [jnp.where(zero, -own[s], other[s]) for s in range(n)]
    v = [own[s] + other[(s - 1) % n] for s in range(n)]
    half = range(1, (n + 1) // 2)
    even = {0: v[0]}
    odd = {}
    if n % 2 == 0:
        even[n // 2] = v[n // 2]
    for x in half:
        even[x] = v[x] + v[n - x]
        odd[x] = v[x] - v[n - x]
    back_even = {x: None for x in even}
    back_odd = {x: None for x in odd}
    for k in range(n):
        is_sine = abs(basis[k, 0]) < 1e-9
        source, target = (odd, back_odd) if is_sine else (even, back_even)
        mode = None
        for x in source:
            term = float(basis[k, x]) * source[x]
            mode = term if mode is None else mode + term
        mode = mode * weight_ref[plan.levels.index(np.round(plan.moment[k], 9))]
        for x in target:
            term = float(basis[k, x]) * mode
            target[x] = term if target[x] is None else target[x] + term
    out = [None] * n
    for x in back_even:
        out[x] = back_even[x]
    for x in half:
        out[x] = back_even[x] + back_odd[x]
        out[n - x] = back_even[x] - back_odd[x]
    out = [value + shift for value in out]
    for d in range(n):
        send_ref[g, d, 0] = out[d]
        send_ref[g, d, 1] = out[(d + 1) % n]


def gauge_of(slab_ref, planes, gauge_ref):
    rows = gauge_ref.shape[2]

    for p in range(planes + 1):

        @pl.loop(0, rows // 8)
        def _(j):
            band = pl.ds(pl.multiple_of(j * 8, 8), 8)
            g = exponential([slab_ref[f * (planes + 1) + p, band, :] for f in range(FIELDS)])
            for a in range(3):
                for b in range(3):
                    for part in range(2):
                        gauge_ref[at(part, a, b), p, band, :] = g[a][b][part]


def shift_all(planes, gauge_ref, ahead_ref):
    for e in range(18):
        for p in range(planes):
            ahead_ref[e, p] = y_ahead(gauge_ref[e, p])
            ahead_ref[18 + e, p] = z_ahead(gauge_ref[e, p])


def rotate_plane(get_band, put_band, p, gauge_ref, ahead_ref):
    rows = gauge_ref.shape[2]

    @pl.loop(0, rows // 8)
    def _(j):
        start = pl.multiple_of(j * 8, 8)
        band = pl.ds(start, 8)
        for i in range(3):
            g = [
                [tuple(gauge_ref[at(r, a, b), p, band, :] for r in range(2)) for b in range(3)]
                for a in range(3)
            ]
            u = [
                [tuple(get_band(i, r, a, b, p, j) for r in range(2)) for b in range(3)]
                for a in range(3)
            ]
            if i == 0:
                source = lambda r, a, b: gauge_ref[at(r, a, b), p + 1, band, :]
            else:
                source = lambda r, a, b: ahead_ref[(i - 1) * 18 + at(r, a, b), p, band, :]
            ahead = [
                [tuple(source(r, a, b) for r in range(2)) for b in range(3)]
                for a in range(3)
            ]
            out = matmul3(matmul3(g, u), ahead, adjoint=True)
            for a in range(3):
                for b in range(3):
                    for r in range(2):
                        put_band(i, r, a, b, p, j, out[a][b][r])


class Steps:
    def __init__(self, relay, start, gap, hop):
        self.relay, self.start, self.gap, self.hop = relay, start, gap, hop
        chunks = relay.up.shape[0]
        self.left = sorted(
            [(k, h) for k in range(chunks) for h in range(1, relay.deep)], key=self.ready
        )

    def ready(self, step):
        return self.start + self.gap * step[0] + self.hop * step[1]

    def until(self, time, keep=0):
        while len(self.left) > keep and self.ready(self.left[0]) <= time:
            self.relay.step(*self.left.pop(0))


class Gather:
    def __init__(self, sizes, axes, target, send, recv):
        self.axes, self.target, self.send, self.recv = axes, target, send, recv
        me = [lax.axis_index(axis) for axis in axes]
        extent = [sizes[axis] for axis in axes]
        slot = 0
        for index, size in zip(me, extent):
            slot = slot * size + index
        self.slot = slot
        self.peers = []
        for flat in range(1, math.prod(extent)):
            rest, peer = flat, {}
            for axis, index, size in reversed(list(zip(axes, me, extent))):
                peer[axis] = lax.rem(index + rest % size, size)
                rest //= size
            self.peers.append((flat, peer))

    def run(self, source):
        copies = []
        for flat, peer in self.peers:
            copies.append(
                pltpu.make_async_remote_copy(
                    src_ref=source,
                    dst_ref=self.target.at[self.slot],
                    send_sem=self.send.at[flat],
                    recv_sem=self.recv.at[flat],
                    device_id=peer,
                    device_id_type=MESH,
                )
            )
            copies[-1].start()
        self.target[self.slot] = source[...]
        for copy in copies:
            copy.wait()


def main_kernel(
    plan, stages, sink_any, src_any, site_any, links_any, right_any, left_any, back_any,
    turn_any, yz_any, prop_any,
    out_ref, table_ref,
    sink_ref, src_ref, site_ref,
    links_ref, right_ref, left_ref, back_ref, turn_ref, yz_ref, prop_ref, load_sems,
    send_ref, recv_ref, swap_sems, weight_ref, ratio_ref, odd_ref, slab_one, slab_two, lattice_ref,
    gauge_ref, ahead_ref, up_one, down_one, sems_one, up_two, down_two, sems_two, acc_ref, sum_ref, row_ref, *gathers,
):
    planes, rows, sizes = plan.planes, plan.rows, plan.sizes
    space, times = sizes["space"], sizes["tm"]
    stages = [
        Gather(sizes, axes, *gathers[3 * i : 3 * i + 3]) for i, axes in enumerate(stages)
    ]
    total = greet(sizes)

    pairs_of = [
        (right_any, right_ref), (left_any, left_ref), (yz_any, yz_ref),
        (back_any, back_ref), (turn_any, turn_ref), (sink_any, sink_ref), (src_any, src_ref),
        (site_any, site_ref), (prop_any, prop_ref),
    ]
    early = [
        pltpu.make_async_copy(
            links_any.at[pl.ds(i * 18, 18)], links_ref.at[pl.ds(i * 18, 18)], load_sems.at[i]
        )
        for i in range(3)
    ]
    late = [
        pltpu.make_async_copy(a, b, load_sems.at[3 + i]) for i, (a, b) in enumerate(pairs_of)
    ]
    early += late[:3]
    late = late[3:]
    for copy in early + late:
        copy.start()

    swaps = [
        Swap(space, send_ref.at[i], recv_ref.at[i], swap_sems.at[2 * i], swap_sems.at[2 * i + 1])
        for i in range(2 * ITERS)
    ]

    def own_one(k, j, band=slice(None)):
        g, p = divmod(k, planes)
        return slab_one[(g * plan.ratio + j) * (planes + 1) + p, band, :]

    def own_two(k, j, band=slice(None)):
        f, p = divmod(k, planes)
        return slab_two[f * (planes + 1) + p, band, :]

    relays = [
        Relay(times, sink_ref, own_one, up_one, down_one, sems_one),
        Relay(times, sink_ref, own_two, up_two, down_two, sems_two),
    ]
    steps = [Steps(relays[0], 1.5, 0.7, 3.5), Steps(relays[1], 0.6, 0.35, 3.0)]

    def sweep(u, index, before=lambda: None):
        one, two = swaps[2 * index], swaps[2 * index + 1]
        slab, relay = (slab_one, slab_two)[index], relays[index]
        for g in range(plan.groups):
            forward(plan, u, g, right_ref[...], left_ref[...], ratio_ref, odd_ref, one.send)
            if g == 0:
                before()
            one.start(g)
            if index:
                steps[0].until(5.5 + 0.3 * g)
        if index == 0:
            for copy in late[:-1]:
                copy.wait()
            weigh(plan, yz_ref, weight_ref)
        for g in range(plan.groups):
            if index:
                steps[0].until(9.3 + 0.7 * g)
            one.arrive(g)
            across(plan, g, one.recv, weight_ref, two.send)
            two.start(g)
        for g in range(plan.groups):
            if index:
                steps[0].until(13.0 + 0.7 * g)
            two.arrive(g)
            backward(
                plan, g, back_ref[...], turn_ref[...], ratio_ref, odd_ref, two.recv, slab
            )
            count = planes * (plan.ratio if index else 1)
            for k in range(count):
                relay.step(g * count + k, 0)

    for copy in early:
        copy.wait()
    ratio_ref[...] = 1.0 / (yz_ref[...] + 2.0)

    def first(i, part, a, b, p):
        return links_ref[i * 18 + at(part, a, b), pl.ds(p, rows, planes), :]

    sweep(first, 0, lambda: pl.semaphore_wait(pltpu.get_barrier_semaphore(), total))
    steps[0].until(2.5)
    gauge_of(slab_one, planes, gauge_ref)
    steps[0].until(3.2)
    shift_all(planes, gauge_ref, ahead_ref)

    def get(i, r, a, b, p, j):
        return links_ref[i * 18 + at(r, a, b), pl.ds(j * 8 * planes + p, 8, planes), :]

    def put(i, r, a, b, p, j, value):
        lattice_ref[i * 18 + at(r, a, b), p, pl.ds(pl.multiple_of(j * 8, 8), 8), :] = value

    for p in range(planes):
        rotate_plane(get, put, p, gauge_ref, ahead_ref)
        steps[0].until(4.3 + 0.7 * p)

    sweep(lambda i, part, a, b, p: lattice_ref[i * 18 + at(part, a, b), p], 1)

    time = [2.5]

    def pause(length):
        time[0] += length
        steps[1].until(time[0])

    pause(0.0)
    gauge_of(slab_two, planes, gauge_ref)
    pause(0.7)
    shift_all(planes, gauge_ref, ahead_ref)
    pause(0.4)

    def get_last(i, r, a, b, p, j):
        return lattice_ref[i * 18 + at(r, a, b), p, pl.ds(pl.multiple_of(j * 8, 8), 8), :]

    def put_last(i, r, a, b, p, j, value):
        out_ref[i * 18 + at(r, a, b), pl.ds(j * 8 * planes + p, 8, planes), :] = value

    for p in range(planes):
        rotate_plane(get_last, put_last, p, gauge_ref, ahead_ref)
        pause(0.7)
    steps[0].until(1e9)
    for p in range(planes):

        @pl.loop(0, rows // 8)
        def _(j):
            band = pl.ds(pl.multiple_of(j * 8, 8), 8)
            one = exponential(
                [
                    relays[0].value((f // plan.ratio) * planes + p, f % plan.ratio, band)
                    for f in range(FIELDS)
                ]
            )
            for a in range(3):
                for b in range(3):
                    for part in range(2):
                        ahead_ref[at(part, a, b), p, band, :] = one[a][b][part]

    pause(0.6)
    for swap in swaps:
        swap.drain()
    acc_ref[...] = jnp.zeros_like(acc_ref)
    sum_ref[...] = jnp.zeros_like(sum_ref)
    site = site_ref[0]
    column = lax.rem(site, rows * LANES)
    plane = lax.div(site, rows * LANES) - lax.axis_index("space") * planes
    present = lax.rem(src_ref[0], times) == lax.axis_index("tm")
    present = present & (plane >= 0) & (plane < planes)
    spot = (lax.broadcasted_iota(jnp.int32, (rows, LANES), 0) == lax.div(column, LANES)) & (
        lax.broadcasted_iota(jnp.int32, (rows, LANES), 1) == lax.rem(column, LANES)
    )

    def pick(ref, f):
        value = jnp.zeros((rows, LANES), jnp.float32)
        for p in range(planes):
            here = spot & (plane == p)
            value = value + jnp.where(here, ref[f * (planes + 1) + p], 0.0)
        value = jnp.sum(jnp.sum(value, axis=0, keepdims=True), axis=1, keepdims=True)
        return jnp.broadcast_to(value, (8, LANES))

    anchor = matmul3(
        exponential([pick(slab_two, f) for f in range(FIELDS)]),
        exponential([pick(slab_one, f) for f in range(FIELDS)]),
    )
    pairs = prop_ref.shape[0] // 2
    first_lane = lane_of((1, LANES)) == 0
    for r in range(2):
        for a in range(3):
            for b in range(3):
                e = 2 * pairs + at(r, a, b)
                sum_ref[e : e + 1, :] = jnp.where(
                    first_lane & present, anchor[a][b][r][0:1, :], 0.0
                )
    late[-1].wait()
    pause(1e9) if times == 1 else None
    for p in range(planes):
        steps[1].until(1e9, keep=planes - 1 - p)

        @pl.loop(0, rows // 8)
        def _(j):
            band = pl.ds(pl.multiple_of(j * 8, 8), 8)
            two = exponential(
                [
                    relays[1].value(f * planes + p, 0, band)
                    for f in range(FIELDS)
                ]
            )
            one = [
                [tuple(ahead_ref[at(r, a, b), p, band, :] for r in range(2)) for b in range(3)]
                for a in range(3)
            ]
            t = matmul3(two, one)
            for q in range(pairs // 3):
                s = [
                    tuple(
                        prop_ref[r * pairs + q * 3 + k, pl.ds(j * 8 * planes + p, 8, planes), :]
                        for r in range(2)
                    )
                    for k in range(3)
                ]
                for a in range(3):
                    re = im = None
                    for k in range(3):
                        x = cmul(t[a][k], s[k])
                        re, im = x if re is None else (re + x[0], im + x[1])
                    acc_ref[q * 3 + a] += re
                    acc_ref[pairs + q * 3 + a] += im

    for e in range(2 * pairs):
        sum_ref[e : e + 1, :] = jnp.sum(acc_ref[e], axis=0, keepdims=True)
    total = sum_ref[...]
    high = total.astype(jnp.bfloat16)
    low = (total - high.astype(jnp.float32)).astype(jnp.bfloat16)
    row_ref[...] = lax.dot_general(
        jnp.ones((16, 2 * LANES), jnp.bfloat16),
        jnp.concatenate([high, low], axis=1),
        (((1,), (1,)), ((), ())),
        preferred_element_type=jnp.float32,
    )[0:1, :]
    stages[0].run(row_ref)
    if len(stages) == 1:
        for t in range(times):
            value = stages[0].target[t]
            for s in range(1, space):
                value = value + stages[0].target[s * times + t]
            table_ref[t : t + 1, :] = value
    else:
        value = stages[0].target[0]
        for s in range(1, space):
            value = value + stages[0].target[s]
        row_ref[...] = value
        stages[1].run(row_ref)
        for t in range(times):
            table_ref[t : t + 1, :] = stages[1].target[t]
    for relay in relays:
        relay.drain()


def close_kernel(pairs, scale, final_ref, table_ref, out_ref, wall_ref, flat_ref, sem):
    share = final_ref.shape[0] // PIECES
    copies = [
        pltpu.make_async_copy(
            final_ref.at[pl.ds(i * share, share)], out_ref.at[pl.ds(i * share, share)], sem.at[i]
        )
        for i in range(PIECES)
    ]
    for copy in copies:
        copy.start()
    times = table_ref.shape[0]
    flat_ref[...] = jnp.zeros_like(flat_ref)
    for t in range(times):
        for r in range(2):
            flat_ref[r : r + 1, t * pairs : (t + 1) * pairs] = table_ref[
                t : t + 1, r * pairs : (r + 1) * pairs
            ]
    length = flat_ref.shape[1]
    entry = jnp.sum(table_ref[...], axis=0, keepdims=True)
    lanes = lax.broadcasted_iota(jnp.int32, (1, length), 1)
    colour = lax.rem(lax.div(lanes, SC), 3)
    re, im = flat_ref[0:1, :], flat_ref[1:2, :]
    real = imag = jnp.zeros((1, length), jnp.float32)
    for gap in range(-2, 3):
        xr = pltpu.roll(re, (gap * SC) % length, 1) if gap else re
        xi = pltpu.roll(im, (gap * SC) % length, 1) if gap else im
        for b in range(3):
            c = b - gap
            if 0 <= c < 3:
                ar, ai = (
                    jnp.broadcast_to(
                        entry[:, 2 * pairs + at(r, b, c) : 2 * pairs + at(r, b, c) + 1],
                        (1, length),
                    )
                    for r in range(2)
                )
                real = real + jnp.where(colour == b, xr * ar + xi * ai, 0.0)
                imag = imag + jnp.where(colour == b, xi * ar - xr * ai, 0.0)
    wall_ref[0:1, :] = real[:, : SC * SC] * scale
    wall_ref[1:2, :] = imag[:, : SC * SC] * scale
    for copy in copies:
        copy.wait()


def body(sizes, links, propagator, sink_time, src_time, src_site):
    space, times = sizes["space"], sizes["tm"]
    planes, area = links.shape[5], links.shape[6]
    side = math.isqrt(area)
    wide = planes * space
    rows = area // LANES
    assert side * 2 == LANES and rows % 8 == 0

    basis, moment = real_basis(side)
    right, left = plane_matrices(basis)
    back, turn = plane_matrices(basis.T)
    x_basis, x_moment = real_basis(space)
    yz = (moment.reshape(rows, 2, 1) + moment[None, None, :]).reshape(rows, LANES)
    yz = yz.astype(np.float32)
    plan = Plan(sizes, planes, rows, x_basis, x_moment)

    def fold(x):
        lead = x.shape[:-2]
        x = x.reshape(lead + (planes, rows, LANES))
        return jnp.swapaxes(x, -3, -2).reshape((-1, rows * planes, LANES))

    linked, source = fold(links[0]), fold(propagator)
    pairs = propagator.shape[1]
    assert 2 * pairs + 18 <= LANES
    stages = [("space", "tm")] if space * times <= 64 else [("space",), ("tm",)]
    vmem = lambda *shape: pltpu.VMEM(shape, jnp.float32)
    sems = pltpu.SemaphoreType.DMA
    chunks = plan.groups * planes
    gathers = []
    for axes in stages:
        count = math.prod(sizes[axis] for axis in axes)
        gathers += [vmem(count, 1, LANES), sems((count,)), sems((count,))]
    tables = [right, left, back, turn]
    scratch = [pltpu.SMEM((1,), jnp.int32)] * 3 + [vmem(*linked.shape)]
    scratch += [pltpu.VMEM(m.shape, jnp.bfloat16) for m in tables]
    scratch += [vmem(*yz.shape), vmem(*source.shape), sems((12,))]
    scratch += [vmem(2 * ITERS, *plan.chunk)] * 2
    scratch += [sems((4 * ITERS, plan.groups, space)), vmem(len(plan.levels), 8, LANES)]
    scratch += [vmem(*yz.shape), vmem(FIELDS, rows, LANES)]
    scratch += [vmem(*plan.slab)] * 2 + [vmem(54, planes, rows, LANES)]
    scratch += [vmem(18, planes + 1, rows, LANES), vmem(36, planes, rows, LANES)]
    scratch += [vmem(chunks, plan.ratio, rows, LANES)] * 2 + [sems((4, chunks))]
    chunks = FIELDS * planes
    scratch += [vmem(chunks, 1, rows, LANES)] * 2 + [sems((4, chunks))]
    scratch += [vmem(2 * pairs, 8, LANES), vmem(LANES, LANES), vmem(1, LANES)]
    final, table = pl.pallas_call(
        functools.partial(main_kernel, plan, stages),
        out_shape=[
            pltpu.VMEM(linked.shape, jnp.float32),
            pltpu.VMEM((times, LANES), jnp.float32),
        ],
        in_specs=[HBM] * 10,
        out_specs=[VMEM] * 2,
        scratch_shapes=scratch + gathers,
        compiler_params=pltpu.CompilerParams(
            collective_id=0, has_side_effects=True, vmem_limit_bytes=LIMIT
        ),
    )(sink_time, src_time, src_site, linked, *tables, yz, source)
    final, wall = pl.pallas_call(
        functools.partial(close_kernel, pairs, float(wide * area) ** (-0.5)),
        out_shape=[
            jax.ShapeDtypeStruct(linked.shape, jnp.float32),
            jax.ShapeDtypeStruct((2, SC * SC), jnp.float32),
        ],
        in_specs=[VMEM] * 2,
        out_specs=[HBM, VMEM],
        scratch_shapes=[vmem(8, 2 * LANES), sems((PIECES,))],
    )(*(pltpu.with_memory_space_constraint(x, pltpu.VMEM) for x in (final, table)))
    final = jnp.swapaxes(final.reshape(54, rows, planes, LANES), 1, 2)
    return final.reshape(links.shape), wall


def solution(mesh):
    sizes = {axis: mesh.shape[axis] for axis in ("space", "tm")}
    placed = (
        P("tm", None, None, None, None, "space", None),
        P(None, "tm", "space", None),
        P(),
        P(),
        P(),
    )
    return jax.shard_map(
        functools.partial(body, sizes),
        mesh=mesh,
        in_specs=placed,
        out_specs=(P("tm", None, None, None, None, "space", None), P()),
        check_vma=False,
    )
```

```python
import functools
import math

import jax
import jax.numpy as jnp
import numpy as np
from jax import lax
from jax.experimental import pallas as pl
from jax.experimental.pallas import tpu as pltpu
from jax.sharding import PartitionSpec as P

SC = 12
ITERS = 2
STEP = 0.08 / 16.0
PEAK = 12.0
LANES = 128
FIELDS = 8
PIECES = 6
EXACT = lax.Precision.HIGHEST
MESH = pl.DeviceIdType.MESH
VMEM = pl.BlockSpec(memory_space=pltpu.VMEM)
HBM = pl.BlockSpec(memory_space=pltpu.HBM)
LIMIT = 60 * 1024 * 1024


def real_basis(n):
    x = np.arange(n)
    rows, moment = [], []
    for k in range(n // 2 + 1):
        angle = 2.0 * np.pi * ((k * x) % n) / n
        square = 4.0 * np.sin(np.pi * k / n) ** 2
        if k == 0 or 2 * k == n:
            rows.append(np.cos(angle) / np.sqrt(n))
            moment.append(square)
        else:
            rows.append(np.cos(angle) * np.sqrt(2.0 / n))
            rows.append(np.sin(angle) * np.sqrt(2.0 / n))
            moment += [square, square]
    return np.array(rows), np.array(moment)


def halves(m):
    high = m.astype(jnp.bfloat16)
    return high, (m - high.astype(np.float64)).astype(jnp.bfloat16)


def plane_matrices(q):
    n = q.shape[0]
    zero = np.zeros((n, n))
    right = np.block([[q.T, zero, zero, q.T], [zero, q.T, q.T, zero]])
    even, odd = q[0::2], q[1::2]
    left = np.block([[even[:, 0::2], even[:, 1::2]], [odd[:, 1::2], odd[:, 0::2]]])
    high, low = halves(right)
    right = np.concatenate([high, high, low], axis=0)
    high, low = halves(left)
    return right, np.concatenate([high, high, low], axis=1)


def triple(x, axis):
    high = x.astype(jnp.bfloat16)
    low = (x - high.astype(jnp.float32)).astype(jnp.bfloat16)
    return jnp.concatenate([high, low, high], axis=axis)


def dot(a, b):
    return jnp.dot(a, b, preferred_element_type=jnp.float32)


def plane_transform(slabs, right, left):
    rows = slabs[0].shape[0]
    wide = dot(triple(jnp.concatenate(slabs, axis=0), 1), right)
    count = len(slabs)
    straight = [wide[i * rows : (i + 1) * rows, :LANES] for i in range(count)]
    swapped = [wide[i * rows : (i + 1) * rows, LANES:] for i in range(count)]
    tall = jnp.concatenate(
        [jnp.concatenate(straight, axis=1), jnp.concatenate(swapped, axis=1)], axis=0
    )
    both = dot(left, triple(tall, 0))
    low = lax.broadcasted_iota(jnp.int32, (rows, LANES), 1) < LANES // 2
    return [
        jnp.where(
            low,
            both[:rows, i * LANES : (i + 1) * LANES],
            both[rows:, i * LANES : (i + 1) * LANES],
        )
        for i in range(count)
    ]


def lane_of(shape):
    return lax.broadcasted_iota(jnp.int32, shape, 1)


def y_behind(v):
    half = LANES // 2
    r = pltpu.roll(v, half, 1)
    return jnp.where(lane_of(v.shape) < half, pltpu.roll(r, 1, 0), r)


def y_ahead(v):
    half = LANES // 2
    r = pltpu.roll(v, half, 1)
    return jnp.where(lane_of(v.shape) < half, r, pltpu.roll(r, v.shape[0] - 1, 0))


def z_behind(v):
    half = LANES // 2
    edge = lane_of(v.shape) % half == 0
    return jnp.where(edge, pltpu.roll(v, half + 1, 1), pltpu.roll(v, 1, 1))


def z_ahead(v):
    half = LANES // 2
    edge = lane_of(v.shape) % half == half - 1
    return jnp.where(edge, pltpu.roll(v, half - 1, 1), pltpu.roll(v, LANES - 1, 1))


PAIRS = ((0, 1), (0, 2), (1, 2))


def project(get, f):
    if f < 6:
        a, b = PAIRS[f % 3]
        if f < 3:
            return 0.5 * (get(0, a, b) - get(0, b, a))
        return 0.5 * (get(1, a, b) + get(1, b, a))
    diag = [get(1, a, a) for a in range(3)]
    return diag[f - 6] - (diag[0] + diag[1] + diag[2]) * (1.0 / 3.0)


def cmul(a, b):
    return (a[0] * b[0] - a[1] * b[1], a[0] * b[1] + a[1] * b[0])


def exponential(fields):
    v = [STEP * f for f in fields]
    h0, h1 = v[6], v[7]
    h2 = -(h0 + h1)
    h01, h02, h12 = (v[3], -v[0]), (v[4], -v[1]), (v[5], -v[2])
    n01 = h01[0] * h01[0] + h01[1] * h01[1]
    n02 = h02[0] * h02[0] + h02[1] * h02[1]
    n12 = h12[0] * h12[0] + h12[1] * h12[1]
    c = 0.5 * (h0 * h0 + h1 * h1 + h2 * h2) + n01 + n02 + n12
    prod = cmul(h01, h12)
    triple = prod[0] * h02[0] + prod[1] * h02[1]
    d = h0 * h1 * h2 + 2.0 * triple - h0 * n12 - h1 * n02 - h2 * n01
    cd, cc, dd = c * d, c * c, d * d
    f0 = (1.0 - dd * (1 / 720), cd * (1 / 120) - d * (1 / 6))
    f1 = (d * (1 / 24) - cd * (1 / 360), 1.0 - c * (1 / 6) + cc * (1 / 120))
    f2 = (c * (1 / 24) - 0.5 - cc * (1 / 720), d * (1 / 120))
    for _ in range(3):
        s00, s01, s02 = cmul(f0, f0), cmul(f0, f1), cmul(f0, f2)
        s11, s12, s22 = cmul(f1, f1), cmul(f1, f2), cmul(f2, f2)
        f0 = tuple(s00[i] + 2.0 * d * s12[i] for i in range(2))
        f1 = tuple(2.0 * (s01[i] + c * s12[i]) + d * s22[i] for i in range(2))
        f2 = tuple(s11[i] + 2.0 * s02[i] + c * s22[i] for i in range(2))
    conj = lambda x: (x[0], -x[1])
    mixed = cmul(h02, conj(h12))
    q01 = (mixed[0] - h2 * h01[0], mixed[1] - h2 * h01[1])
    q02 = (prod[0] - h1 * h02[0], prod[1] - h1 * h02[1])
    mixed = cmul(conj(h01), h02)
    q12 = (mixed[0] - h0 * h12[0], mixed[1] - h0 * h12[1])
    diag = ((h0, h0 * h0 + n01 + n02), (h1, h1 * h1 + n01 + n12), (h2, h2 * h2 + n02 + n12))
    gauge = [[None] * 3 for _ in range(3)]
    for a in range(3):
        h, q = diag[a]
        gauge[a][a] = tuple(f0[i] + f1[i] * h + f2[i] * q for i in range(2))
    for a, b, h, q in ((0, 1, h01, q01), (0, 2, h02, q02), (1, 2, h12, q12)):
        x, y = cmul(f1, h), cmul(f2, q)
        gauge[a][b] = (x[0] + y[0], x[1] + y[1])
        x, y = cmul(f1, conj(h)), cmul(f2, conj(q))
        gauge[b][a] = (x[0] + y[0], x[1] + y[1])
    return gauge


def matmul3(left, right, adjoint=False):
    out = [[None] * 3 for _ in range(3)]
    for a in range(3):
        for b in range(3):
            re = im = None
            for k in range(3):
                xr, xi = left[a][k]
                yr, yi = right[b][k] if adjoint else right[k][b]
                if adjoint:
                    r, i = xr * yr + xi * yi, xi * yr - xr * yi
                else:
                    r, i = xr * yr - xi * yi, xr * yi + xi * yr
                re, im = (r, i) if re is None else (re + r, im + i)
            out[a][b] = (re, im)
    return out


def at(part, a, b):
    return part * 9 + a * 3 + b


class Swap:
    def __init__(self, size, send, recv, send_sem, recv_sem):
        self.size, self.send, self.recv = size, send, recv
        self.send_sem, self.recv_sem = send_sem, recv_sem
        self.me = lax.axis_index("space")

    def copy(self, g, off):
        peer = lax.rem(self.me + off, self.size)
        return pltpu.make_async_remote_copy(
            src_ref=self.send.at[g, peer],
            dst_ref=self.recv.at[g, self.me],
            send_sem=self.send_sem.at[g, off],
            recv_sem=self.recv_sem.at[g, off],
            device_id={"space": peer},
            device_id_type=MESH,
        )

    def start(self, g):
        for off in range(1, self.size):
            self.copy(g, off).start()
        self.recv[g, self.me] = self.send[g, self.me]

    def arrive(self, g):
        for off in range(1, self.size):
            self.copy(g, off).wait_recv()

    def drain(self):
        for g in range(self.send.shape[0]):
            for off in range(1, self.size):
                self.copy(g, off).wait_send()


class Relay:
    def __init__(self, size, root, own, up, down, sems):
        self.size, self.root, self.own = size, root, own
        self.up, self.down = up, down
        self.sems = sems
        self.me = lax.axis_index("tm")
        self.deep = min(size, 4)

    def hop(self, k, rise):
        buffer = self.up if rise else self.down
        base = 0 if rise else 2
        step = 1 if rise else self.size - 1
        return pltpu.make_async_remote_copy(
            src_ref=buffer.at[k],
            dst_ref=buffer.at[k],
            send_sem=self.sems.at[base, k],
            recv_sem=self.sems.at[base + 1, k],
            device_id={"tm": lax.rem(self.me + step, self.size)},
            device_id_type=MESH,
        )

    def step(self, k, h):
        for rise in (True, False):
            place = self.me if rise else self.size - 1 - self.me
            last = h == self.deep - 1
            here = (place >= h) if last else (place == h)
            buffer = self.up if rise else self.down
            parts = buffer.shape[1]

            @pl.when(here)
            def _():
                if h == 0:
                    for j in range(parts):
                        buffer[k, j] = self.own(k, j)
                else:
                    self.hop(k, rise).wait_recv()
                    mine = jnp.broadcast_to(lax.rem(self.root[0], self.size), buffer.shape[2:]) == self.me
                    for j in range(parts):
                        buffer[k, j] = jnp.where(mine, self.own(k, j), buffer[k, j])
                if not last:
                    self.hop(k, rise).start()
                elif self.size > self.deep:

                    @pl.when(place < self.size - 1)
                    def _():
                        self.hop(k, rise).start()

    def drain(self):
        for k in range(self.up.shape[0]):

            @pl.when(self.me < self.size - 1)
            def _():
                self.hop(k, True).wait_send()

            @pl.when(self.me > 0)
            def _():
                self.hop(k, False).wait_send()

    def value(self, k, j, band):
        own = self.own(k, j, band)
        root = jnp.broadcast_to(lax.rem(self.root[0], self.size), own.shape)
        other = jnp.where(root < self.me, self.up[k, j, band, :], self.down[k, j, band, :])
        return jnp.where(root == self.me, own, other)


def greet(sizes):
    barrier = pltpu.get_barrier_semaphore()
    me, time = lax.axis_index("space"), lax.axis_index("tm")
    size, times = sizes["space"], sizes["tm"]

    def signal(peer):
        pl.semaphore_signal(barrier, inc=1, device_id=peer, device_id_type=MESH)

    for off in range(1, size):
        signal({"space": lax.rem(me + off, size)})
    above, below = time < times - 1, time > 0

    @pl.when(above)
    def _():
        signal({"tm": lax.rem(time + 1, times)})

    @pl.when(below)
    def _():
        signal({"tm": lax.rem(time + times - 1, times)})

    return size - 1 + above.astype(jnp.int32) + below.astype(jnp.int32)


class Plan:
    def __init__(self, sizes, planes, rows, basis, moment):
        self.sizes, self.planes, self.rows = sizes, planes, rows
        self.basis, self.moment = basis, moment
        self.size = sizes["space"]
        self.ratio = 8 * self.size // rows
        self.groups = FIELDS // self.ratio
        assert self.ratio * rows == 8 * self.size and self.groups * self.ratio == FIELDS
        self.levels = sorted(set(np.round(moment, 9)))
        assert planes == 2
        self.chunk = (self.groups, self.size, planes, 8, LANES)
        self.slab = (FIELDS * (planes + 1), rows, LANES)

    def fields(self, g):
        return range(g * self.ratio, (g + 1) * self.ratio)


def weigh(plan, yz_ref, weight_ref):
    block = lax.div(lax.axis_index("space"), plan.ratio)
    yz = yz_ref[pl.ds(pl.multiple_of(block * 8, 8), 8), :]
    above = PEAK * (yz + 2.0)
    base = yz * (yz + 4.0)
    for index, level in enumerate(plan.levels):
        p2 = base + float(level)
        if level == 0.0:
            weight = jnp.where(p2 > 0.0, above / jnp.where(p2 > 0.0, p2, 1.0), 0.0)
        else:
            weight = above / p2
        weight_ref[index] = weight


def origin(shape, block=0):
    row = lax.broadcasted_iota(jnp.int32, shape, 0) + block
    return (row == 0) & (lane_of(shape) == 0)


def forward(plan, u, g, right, left, ratio_ref, odd_ref, send_ref):
    planes = plan.planes
    slabs = []
    for f in plan.fields(g):
        before = None
        for p in range(planes):
            x, y, z = (
                project(lambda part, a, b, i=i: u(i, part, a, b, p), f) for i in range(3)
            )
            value = (y_behind(y) - y + z_behind(z) - z) - x
            slabs.append(value if before is None else value + before)
            before = x
        slabs.append(before)
    done = plane_transform(slabs, right, left)
    ratio = ratio_ref[...]
    for i, f in enumerate(plan.fields(g)):
        even, odd, edge = done[3 * i : 3 * i + 3]
        odd_ref[f] = odd
        share = ratio * odd
        own, other = even + share, jnp.where(origin(odd.shape), odd, edge + share)
        for block in range(plan.rows // 8):
            band = slice(block * 8, block * 8 + 8)
            send_ref[g, block * plan.ratio + i, 0] = own[band, :]
            send_ref[g, block * plan.ratio + i, 1] = other[band, :]


def backward(plan, g, right, left, ratio_ref, odd_ref, recv_ref, slab_ref):
    slabs = []
    ratio = ratio_ref[...]
    for i, f in enumerate(plan.fields(g)):
        here, ahead = (
            jnp.concatenate(
                [recv_ref[g, b * plan.ratio + i, p] for b in range(plan.rows // 8)], axis=0
            )
            for p in range(2)
        )
        slabs += [here, (PEAK * odd_ref[f] + here + ahead) * ratio, ahead]
    base = g * plan.ratio * (plan.planes + 1)
    for index, slab in enumerate(plane_transform(slabs, right, left)):
        slab_ref[base + index] = slab


def across(plan, g, recv_ref, weight_ref, send_ref):
    n, basis = plan.size, plan.basis
    zero = origin((8, LANES), lax.div(lax.axis_index("space"), plan.ratio))
    own = [recv_ref[g, s, 0] for s in range(n)]
    other = [recv_ref[g, s, 1] for s in range(n)]
    shift = other[0]
    for s in range(1, n):
        shift = shift + other[s]
    shift = jnp.where(zero, shift * (-0.25 * PEAK / n), 0.0)
    other = [jnp.where(zero, -own[s], other[s]) for s in range(n)]
    v = [own[s] + other[(s - 1) % n] for s in range(n)]
    half = range(1, (n + 1) // 2)
    even = {0: v[0]}
    odd = {}
    if n % 2 == 0:
        even[n // 2] = v[n // 2]
    for x in half:
        even[x] = v[x] + v[n - x]
        odd[x] = v[x] - v[n - x]
    back_even = {x: None for x in even}
    back_odd = {x: None for x in odd}
    for k in range(n):
        is_sine = abs(basis[k, 0]) < 1e-9
        source, target = (odd, back_odd) if is_sine else (even, back_even)
        mode = None
        for x in source:
            term = float(basis[k, x]) * source[x]
            mode = term if mode is None else mode + term
        mode = mode * weight_ref[plan.levels.index(np.round(plan.moment[k], 9))]
        for x in target:
            term = float(basis[k, x]) * mode
            target[x] = term if target[x] is None else target[x] + term
    out = [None] * n
    for x in back_even:
        out[x] = back_even[x]
    for x in half:
        out[x] = back_even[x] + back_odd[x]
        out[n - x] = back_even[x] - back_odd[x]
    out = [value + shift for value in out]
    for d in range(n):
        send_ref[g, d, 0] = out[d]
        send_ref[g, d, 1] = out[(d + 1) % n]


def gauge_of(slab_ref, planes, gauge_ref, chosen=None):
    rows = gauge_ref.shape[2]

    for p in range(planes + 1) if chosen is None else chosen:

        @pl.loop(0, rows // 8)
        def _(j):
            band = pl.ds(pl.multiple_of(j * 8, 8), 8)
            g = exponential([slab_ref[f * (planes + 1) + p, band, :] for f in range(FIELDS)])
            for a in range(3):
                for b in range(3):
                    for part in range(2):
                        gauge_ref[at(part, a, b), p, band, :] = g[a][b][part]


def shift_all(planes, gauge_ref, ahead_ref):
    for e in range(18):
        for p in range(planes):
            ahead_ref[e, p] = y_ahead(gauge_ref[e, p])
            ahead_ref[18 + e, p] = z_ahead(gauge_ref[e, p])


def rotate_plane(get_band, put_band, p, gauge_ref, ahead_ref, part=0, parts=1):
    bands = gauge_ref.shape[2] // 8

    @pl.loop(part * bands // parts, (part + 1) * bands // parts)
    def _(j):
        start = pl.multiple_of(j * 8, 8)
        band = pl.ds(start, 8)
        for i in range(3):
            g = [
                [tuple(gauge_ref[at(r, a, b), p, band, :] for r in range(2)) for b in range(3)]
                for a in range(3)
            ]
            u = [
                [tuple(get_band(i, r, a, b, p, j) for r in range(2)) for b in range(3)]
                for a in range(3)
            ]
            if i == 0:
                source = lambda r, a, b: gauge_ref[at(r, a, b), p + 1, band, :]
            else:
                source = lambda r, a, b: ahead_ref[(i - 1) * 18 + at(r, a, b), p, band, :]
            ahead = [
                [tuple(source(r, a, b) for r in range(2)) for b in range(3)]
                for a in range(3)
            ]
            out = matmul3(matmul3(g, u), ahead, adjoint=True)
            for a in range(3):
                for b in range(3):
                    for r in range(2):
                        put_band(i, r, a, b, p, j, out[a][b][r])


class Steps:
    def __init__(self, relay, start, gap, hop):
        self.relay, self.start, self.gap, self.hop = relay, start, gap, hop
        chunks = relay.up.shape[0]
        self.left = sorted(
            [(k, h) for k in range(chunks) for h in range(1, relay.deep)], key=self.ready
        )

    def ready(self, step):
        return self.start + self.gap * step[0] + self.hop * step[1]

    def until(self, time, keep=0):
        while len(self.left) > keep and self.ready(self.left[0]) <= time:
            self.relay.step(*self.left.pop(0))


class Gather:
    def __init__(self, sizes, axes, target, send, recv):
        self.axes, self.target, self.send, self.recv = axes, target, send, recv
        me = [lax.axis_index(axis) for axis in axes]
        extent = [sizes[axis] for axis in axes]
        slot = 0
        for index, size in zip(me, extent):
            slot = slot * size + index
        self.slot = slot
        self.peers = []
        for flat in range(1, math.prod(extent)):
            rest, peer = flat, {}
            for axis, index, size in reversed(list(zip(axes, me, extent))):
                peer[axis] = lax.rem(index + rest % size, size)
                rest //= size
            self.peers.append((flat, peer))

    def run(self, source):
        copies = []
        for flat, peer in self.peers:
            copies.append(
                pltpu.make_async_remote_copy(
                    src_ref=source,
                    dst_ref=self.target.at[self.slot],
                    send_sem=self.send.at[flat],
                    recv_sem=self.recv.at[flat],
                    device_id=peer,
                    device_id_type=MESH,
                )
            )
            copies[-1].start()
        self.target[self.slot] = source[...]
        for copy in copies:
            copy.wait()


def main_kernel(
    plan, stages, sink_any, src_any, site_any, links_any, right_any, left_any, back_any,
    turn_any, yz_any, prop_any,
    out_ref, table_ref,
    sink_ref, src_ref, site_ref,
    links_ref, right_ref, left_ref, back_ref, turn_ref, yz_ref, prop_ref, load_sems,
    send_ref, recv_ref, swap_sems, weight_ref, ratio_ref, odd_ref, slab_one, slab_two, lattice_ref,
    gauge_ref, ahead_ref, up_one, down_one, sems_one, up_two, down_two, sems_two, acc_ref, sum_ref, row_ref, *gathers,
):
    planes, rows, sizes = plan.planes, plan.rows, plan.sizes
    space, times = sizes["space"], sizes["tm"]
    stages = [
        Gather(sizes, axes, *gathers[3 * i : 3 * i + 3]) for i, axes in enumerate(stages)
    ]
    total = greet(sizes)

    pairs_of = [
        (right_any, right_ref), (left_any, left_ref), (yz_any, yz_ref),
        (back_any, back_ref), (turn_any, turn_ref), (sink_any, sink_ref), (src_any, src_ref),
        (site_any, site_ref), (prop_any, prop_ref),
    ]
    early = [
        pltpu.make_async_copy(
            links_any.at[pl.ds(i * 18, 18)], links_ref.at[pl.ds(i * 18, 18)], load_sems.at[i]
        )
        for i in range(3)
    ]
    late = [
        pltpu.make_async_copy(a, b, load_sems.at[3 + i]) for i, (a, b) in enumerate(pairs_of)
    ]
    early += late[:3]
    late = late[3:]
    for copy in early + late:
        copy.start()

    swaps = [
        Swap(space, send_ref.at[i], recv_ref.at[i], swap_sems.at[2 * i], swap_sems.at[2 * i + 1])
        for i in range(2 * ITERS)
    ]

    def own_one(k, j, band=slice(None)):
        g, p = divmod(k, planes)
        return slab_one[(g * plan.ratio + j) * (planes + 1) + p, band, :]

    def own_two(k, j, band=slice(None)):
        f, p = divmod(k, planes)
        return slab_two[f * (planes + 1) + p, band, :]

    relays = [
        Relay(times, sink_ref, own_one, up_one, down_one, sems_one),
        Relay(times, sink_ref, own_two, up_two, down_two, sems_two),
    ]
    steps = [Steps(relays[0], 1.5, 0.7, 3.5), Steps(relays[1], 0.5, 0.35, 2.6)]

    def sweep(u, index, before=lambda: None):
        one, two = swaps[2 * index], swaps[2 * index + 1]
        slab, relay = (slab_one, slab_two)[index], relays[index]
        for g in range(plan.groups):
            forward(plan, u, g, right_ref[...], left_ref[...], ratio_ref, odd_ref, one.send)
            if g == 0:
                before()
            one.start(g)
            if index:
                steps[0].until(5.5 + 0.3 * g)
        if index == 0:
            for copy in late[:-1]:
                copy.wait()
            weigh(plan, yz_ref, weight_ref)
        for g in range(plan.groups):
            if index:
                steps[0].until(9.3 + 0.7 * g)
            one.arrive(g)
            across(plan, g, one.recv, weight_ref, two.send)
            two.start(g)
        for g in range(plan.groups):
            if index:
                steps[0].until(13.0 + 0.7 * g)
            two.arrive(g)
            backward(
                plan, g, back_ref[...], turn_ref[...], ratio_ref, odd_ref, two.recv, slab
            )
            count = planes * (plan.ratio if index else 1)
            for k in range(count):
                relay.step(g * count + k, 0)

    for copy in early:
        copy.wait()
    ratio_ref[...] = 1.0 / (yz_ref[...] + 2.0)

    def first(i, part, a, b, p):
        return links_ref[i * 18 + at(part, a, b), pl.ds(p, rows, planes), :]

    sweep(first, 0, lambda: pl.semaphore_wait(pltpu.get_barrier_semaphore(), total))
    steps[0].until(2.5)
    gauge_of(slab_one, planes, gauge_ref)
    steps[0].until(3.2)
    shift_all(planes, gauge_ref, ahead_ref)

    def get(i, r, a, b, p, j):
        return links_ref[i * 18 + at(r, a, b), pl.ds(j * 8 * planes + p, 8, planes), :]

    def put(i, r, a, b, p, j, value):
        lattice_ref[i * 18 + at(r, a, b), p, pl.ds(pl.multiple_of(j * 8, 8), 8), :] = value

    for p in range(planes):
        rotate_plane(get, put, p, gauge_ref, ahead_ref)
        steps[0].until(4.3 + 0.7 * p)

    sweep(lambda i, part, a, b, p: lattice_ref[i * 18 + at(part, a, b), p], 1)

    time = [2.5]

    def pause(length):
        time[0] += length
        steps[1].until(time[0])

    pause(0.0)
    for p in range(planes + 1):
        gauge_of(slab_two, planes, gauge_ref, [p])
        pause(0.35)
    shift_all(planes, gauge_ref, ahead_ref)
    pause(0.45)

    def get_last(i, r, a, b, p, j):
        return lattice_ref[i * 18 + at(r, a, b), p, pl.ds(pl.multiple_of(j * 8, 8), 8), :]

    def put_last(i, r, a, b, p, j, value):
        out_ref[i * 18 + at(r, a, b), pl.ds(j * 8 * planes + p, 8, planes), :] = value

    for p in range(planes):
        for part in range(2):
            rotate_plane(get_last, put_last, p, gauge_ref, ahead_ref, part, 2)
            pause(0.5)
    steps[0].until(1e9)
    for p in range(planes):

        @pl.loop(0, rows // 8)
        def _(j):
            band = pl.ds(pl.multiple_of(j * 8, 8), 8)
            one = exponential(
                [
                    relays[0].value((f // plan.ratio) * planes + p, f % plan.ratio, band)
                    for f in range(FIELDS)
                ]
            )
            for a in range(3):
                for b in range(3):
                    for part in range(2):
                        ahead_ref[at(part, a, b), p, band, :] = one[a][b][part]

        pause(0.4)

    for swap in swaps:
        swap.drain()
        pause(0.2)
    acc_ref[...] = jnp.zeros_like(acc_ref)
    sum_ref[...] = jnp.zeros_like(sum_ref)
    site = site_ref[0]
    column = lax.rem(site, rows * LANES)
    plane = lax.div(site, rows * LANES) - lax.axis_index("space") * planes
    present = lax.rem(src_ref[0], times) == lax.axis_index("tm")
    present = present & (plane >= 0) & (plane < planes)
    spot = (lax.broadcasted_iota(jnp.int32, (rows, LANES), 0) == lax.div(column, LANES)) & (
        lax.broadcasted_iota(jnp.int32, (rows, LANES), 1) == lax.rem(column, LANES)
    )

    def pick(ref, f):
        value = jnp.zeros((rows, LANES), jnp.float32)
        for p in range(planes):
            here = spot & (plane == p)
            value = value + jnp.where(here, ref[f * (planes + 1) + p], 0.0)
        value = jnp.sum(jnp.sum(value, axis=0, keepdims=True), axis=1, keepdims=True)
        return jnp.broadcast_to(value, (8, LANES))

    anchor = matmul3(
        exponential([pick(slab_two, f) for f in range(FIELDS)]),
        exponential([pick(slab_one, f) for f in range(FIELDS)]),
    )
    pairs = prop_ref.shape[0] // 2
    first_lane = lane_of((1, LANES)) == 0
    for r in range(2):
        for a in range(3):
            for b in range(3):
                e = 2 * pairs + at(r, a, b)
                sum_ref[e : e + 1, :] = jnp.where(
                    first_lane & present, anchor[a][b][r][0:1, :], 0.0
                )
    late[-1].wait()
    pause(1e9) if times == 1 else None
    for p in range(planes):
        steps[1].until(1e9, keep=planes - 1 - p)

        @pl.loop(0, rows // 8)
        def _(j):
            band = pl.ds(pl.multiple_of(j * 8, 8), 8)
            two = exponential(
                [
                    relays[1].value(f * planes + p, 0, band)
                    for f in range(FIELDS)
                ]
            )
            one = [
                [tuple(ahead_ref[at(r, a, b), p, band, :] for r in range(2)) for b in range(3)]
                for a in range(3)
            ]
            t = matmul3(two, one)
            for q in range(pairs // 3):
                s = [
                    tuple(
                        prop_ref[r * pairs + q * 3 + k, pl.ds(j * 8 * planes + p, 8, planes), :]
                        for r in range(2)
                    )
                    for k in range(3)
                ]
                for a in range(3):
                    re = im = None
                    for k in range(3):
                        x = cmul(t[a][k], s[k])
                        re, im = x if re is None else (re + x[0], im + x[1])
                    acc_ref[q * 3 + a] += re
                    acc_ref[pairs + q * 3 + a] += im

    for e in range(2 * pairs):
        sum_ref[e : e + 1, :] = jnp.sum(acc_ref[e], axis=0, keepdims=True)
    total = sum_ref[...]
    high = total.astype(jnp.bfloat16)
    low = (total - high.astype(jnp.float32)).astype(jnp.bfloat16)
    row_ref[...] = lax.dot_general(
        jnp.ones((16, 2 * LANES), jnp.bfloat16),
        jnp.concatenate([high, low], axis=1),
        (((1,), (1,)), ((), ())),
        preferred_element_type=jnp.float32,
    )[0:1, :]
    stages[0].run(row_ref)
    if len(stages) == 1:
        for t in range(times):
            value = stages[0].target[t]
            for s in range(1, space):
                value = value + stages[0].target[s * times + t]
            table_ref[t : t + 1, :] = value
    else:
        value = stages[0].target[0]
        for s in range(1, space):
            value = value + stages[0].target[s]
        row_ref[...] = value
        stages[1].run(row_ref)
        for t in range(times):
            table_ref[t : t + 1, :] = stages[1].target[t]
    for relay in relays:
        relay.drain()


def close_kernel(pairs, scale, final_ref, table_ref, out_ref, wall_ref, flat_ref, sem):
    share = final_ref.shape[0] // PIECES
    copies = [
        pltpu.make_async_copy(
            final_ref.at[pl.ds(i * share, share)], out_ref.at[pl.ds(i * share, share)], sem.at[i]
        )
        for i in range(PIECES)
    ]
    for copy in copies:
        copy.start()
    times = table_ref.shape[0]
    flat_ref[...] = jnp.zeros_like(flat_ref)
    for t in range(times):
        for r in range(2):
            flat_ref[r : r + 1, t * pairs : (t + 1) * pairs] = table_ref[
                t : t + 1, r * pairs : (r + 1) * pairs
            ]
    length = flat_ref.shape[1]
    entry = jnp.sum(table_ref[...], axis=0, keepdims=True)
    lanes = lax.broadcasted_iota(jnp.int32, (1, length), 1)
    colour = lax.rem(lax.div(lanes, SC), 3)
    re, im = flat_ref[0:1, :], flat_ref[1:2, :]
    real = imag = jnp.zeros((1, length), jnp.float32)
    for gap in range(-2, 3):
        xr = pltpu.roll(re, (gap * SC) % length, 1) if gap else re
        xi = pltpu.roll(im, (gap * SC) % length, 1) if gap else im
        for b in range(3):
            c = b - gap
            if 0 <= c < 3:
                ar, ai = (
                    jnp.broadcast_to(
                        entry[:, 2 * pairs + at(r, b, c) : 2 * pairs + at(r, b, c) + 1],
                        (1, length),
                    )
                    for r in range(2)
                )
                real = real + jnp.where(colour == b, xr * ar + xi * ai, 0.0)
                imag = imag + jnp.where(colour == b, xi * ar - xr * ai, 0.0)
    wall_ref[0:1, :] = real[:, : SC * SC] * scale
    wall_ref[1:2, :] = imag[:, : SC * SC] * scale
    for copy in copies:
        copy.wait()


def body(sizes, links, propagator, sink_time, src_time, src_site):
    space, times = sizes["space"], sizes["tm"]
    planes, area = links.shape[5], links.shape[6]
    side = math.isqrt(area)
    wide = planes * space
    rows = area // LANES
    assert side * 2 == LANES and rows % 8 == 0

    basis, moment = real_basis(side)
    right, left = plane_matrices(basis)
    back, turn = plane_matrices(basis.T)
    x_basis, x_moment = real_basis(space)
    yz = (moment.reshape(rows, 2, 1) + moment[None, None, :]).reshape(rows, LANES)
    yz = yz.astype(np.float32)
    plan = Plan(sizes, planes, rows, x_basis, x_moment)

    def fold(x):
        lead = x.shape[:-2]
        x = x.reshape(lead + (planes, rows, LANES))
        return jnp.swapaxes(x, -3, -2).reshape((-1, rows * planes, LANES))

    linked, source = fold(links[0]), fold(propagator)
    pairs = propagator.shape[1]
    assert 2 * pairs + 18 <= LANES
    stages = [("space", "tm")] if space * times <= 64 else [("space",), ("tm",)]
    vmem = lambda *shape: pltpu.VMEM(shape, jnp.float32)
    sems = pltpu.SemaphoreType.DMA
    chunks = plan.groups * planes
    gathers = []
    for axes in stages:
        count = math.prod(sizes[axis] for axis in axes)
        gathers += [vmem(count, 1, LANES), sems((count,)), sems((count,))]
    tables = [right, left, back, turn]
    scratch = [pltpu.SMEM((1,), jnp.int32)] * 3 + [vmem(*linked.shape)]
    scratch += [pltpu.VMEM(m.shape, jnp.bfloat16) for m in tables]
    scratch += [vmem(*yz.shape), vmem(*source.shape), sems((12,))]
    scratch += [vmem(2 * ITERS, *plan.chunk)] * 2
    scratch += [sems((4 * ITERS, plan.groups, space)), vmem(len(plan.levels), 8, LANES)]
    scratch += [vmem(*yz.shape), vmem(FIELDS, rows, LANES)]
    scratch += [vmem(*plan.slab)] * 2 + [vmem(54, planes, rows, LANES)]
    scratch += [vmem(18, planes + 1, rows, LANES), vmem(36, planes, rows, LANES)]
    scratch += [vmem(chunks, plan.ratio, rows, LANES)] * 2 + [sems((4, chunks))]
    chunks = FIELDS * planes
    scratch += [vmem(chunks, 1, rows, LANES)] * 2 + [sems((4, chunks))]
    scratch += [vmem(2 * pairs, 8, LANES), vmem(LANES, LANES), vmem(1, LANES)]
    final, table = pl.pallas_call(
        functools.partial(main_kernel, plan, stages),
        out_shape=[
            pltpu.VMEM(linked.shape, jnp.float32),
            pltpu.VMEM((times, LANES), jnp.float32),
        ],
        in_specs=[HBM] * 10,
        out_specs=[VMEM] * 2,
        scratch_shapes=scratch + gathers,
        compiler_params=pltpu.CompilerParams(
            collective_id=0, has_side_effects=True, vmem_limit_bytes=LIMIT
        ),
    )(sink_time, src_time, src_site, linked, *tables, yz, source)
    final, wall = pl.pallas_call(
        functools.partial(close_kernel, pairs, float(wide * area) ** (-0.5)),
        out_shape=[
            jax.ShapeDtypeStruct(linked.shape, jnp.float32),
            jax.ShapeDtypeStruct((2, SC * SC), jnp.float32),
        ],
        in_specs=[VMEM] * 2,
        out_specs=[HBM, VMEM],
        scratch_shapes=[vmem(8, 2 * LANES), sems((PIECES,))],
    )(*(pltpu.with_memory_space_constraint(x, pltpu.VMEM) for x in (final, table)))
    final = jnp.swapaxes(final.reshape(54, rows, planes, LANES), 1, 2)
    return final.reshape(links.shape), wall


def solution(mesh):
    sizes = {axis: mesh.shape[axis] for axis in ("space", "tm")}
    placed = (
        P("tm", None, None, None, None, "space", None),
        P(None, "tm", "space", None),
        P(),
        P(),
        P(),
    )
    return jax.shard_map(
        functools.partial(body, sizes),
        mesh=mesh,
        in_specs=placed,
        out_specs=(P("tm", None, None, None, None, "space", None), P()),
        check_vma=False,
    )
```
